256 devices in a mesh: gx: 16 (over z, x_lo), gy: 16 (over y, x_hi, core).
Axes of the slice: x: 4 (x_hi: 2, x_lo: 2; x = x_hi * 2 + x_lo), y: 4, z: 8, core: 2. Of those that a mesh axis runs over, the one named last changes fastest.
Arguments:
- gradient: float32 [2048, 512], P('gx', 'gy'), may hold values from -6 to 6
- stat_old: float32 [2048, 2048], P('gx', 'gy'), may hold values from -1.001 to 1.001, as said below
Outputs:
- statistic: float32 [2048, 2048], P('gx', 'gy')
- inverse_root: float32 [2048, 2048], P('gx', 'gy')
The draws below stay inside these ranges and needn't reach their ends.
Inputs may be any that keep to these rules, and one draw needn't show every extreme that they name: stat_old is symmetric positive semidefinite with unit diagonal, the Gram matrix of 2048 unit-length rows of 512 entries.
All inputs are finite; a program needn't handle non-finite values.
Results may differ from the reference program's by a relative error of at most 0.0003.
Values sent between devices are 32-bit elements.
A program may use at most 64 MiB of HBM per device.

```python
import jax
import jax.numpy as jnp
from jax import lax

NSIDE = 2048
MCOLS = 512


def draw_stat_old(key, part):
    factor = jax.random.normal(key, (NSIDE, NSIDE // 4), jnp.float32)
    lengths = jnp.sqrt(jnp.sum(factor * factor, axis=1, keepdims=True))
    factor = factor / lengths
    return jnp.dot(factor, factor.T, preferred_element_type=jnp.float32, precision=lax.Precision.HIGHEST)


def steps_of(stream_key, dims, pieces, low, high):
    factor_of = 1.0
    for dim, shards_of in pieces:
        draws = jax.random.uniform(jax.random.fold_in(jax.random.fold_in(stream_key, 6), dim), (shards_of,), jnp.float32, low / len(pieces), high / len(pieces))
        factor_of = factor_of * jnp.repeat(jnp.exp(draws), dims[dim] // shards_of).reshape((-1,) + (1,) * (len(dims) - 1 - dim))
    return factor_of


def bell_draw(rng, dims, width, reach, pieces=(), kind=jnp.bfloat16):
    array = jax.random.normal(rng, dims, jnp.float32) * width
    if len(pieces) > 0:
        array = steps_of(rng, dims, pieces, -0.22, 0.18) * array
    return jnp.clip(array, min=-reach, max=reach).astype(kind)


def setup_inputs(seed: int = 0) -> dict:
    key_of = jax.random.split(jax.random.key(seed), 3)
    return {
        "gradient": bell_draw(key_of[0], (NSIDE, MCOLS), 1.0, 6.0, ((0, 16), (1, 16)), jnp.float32),
        "stat_old": draw_stat_old(jax.random.fold_in(key_of[2], 71), 0),
    }


def matmul(leading, trailing):
    return jnp.dot(leading, trailing, preferred_element_type=jnp.float32, precision=lax.Precision.HIGHEST)

def reference(gradient, stat_old):
    statistic = 0.9 * stat_old + matmul(gradient, gradient.T) / MCOLS
    divisor = 2.0 * jnp.sqrt(jnp.sum(statistic * statistic) / NSIDE)
    identity = jnp.eye(NSIDE, dtype=jnp.float32)
    normed = statistic / divisor
    first_step = 1.5 * identity - 0.5 * normed
    root_half = matmul(normed, first_step)
    product_mid = matmul(first_step, root_half)
    second_step = 1.5 * identity - 0.5 * product_mid
    inverse_root = matmul(second_step, first_step)
    return (statistic, inverse_root)
```

```python
import functools

import jax
import jax.numpy as jnp
from jax import lax
from jax.experimental import pallas as pl
from jax.experimental.pallas import tpu as pltpu
from jax.sharding import PartitionSpec as P

MESH = pl.DeviceIdType.MESH
N_GX = 16
N_GY = 16
B = 128
HALF = B // 2
PIECE = 32

COL_KEYS = (
    [("x", 0)]
    + [("z", d, st, h, s) for d in (0, 1) for st in (0, 1) for h in (0, 1) for s in (1, 2, 3, 4)
       if (h == 0 or st == 0) and (s < 4 or (d == 0) == (h == 0))]
    + [("xb", d, s) for d in (0, 1) for s in range(0, 5) if (d == 0 or s > 0) and (s < 4 or d == 1)]
)
ROW_KEYS = (
    [("x", 0)]
    + [("y", d, st, 1) for d in (0, 1) for st in (0, 1)]
    + [("y", d, st, 2) for d in (0, 1) for st in (0, 1)]
    + [("c", st, t) for st in (0, 1) for t in range(4)]
)
COL_AT = {key: number for number, key in enumerate(COL_KEYS)}
ROW_AT = {key: number for number, key in enumerate(ROW_KEYS)}


def split(x):
    high = x.astype(jnp.bfloat16)
    low = (x - high.astype(jnp.float32)).astype(jnp.bfloat16)
    return high, low


def dot3(a, b, dims=(((1,), (0,)), ((), ()))):
    a_high, a_low = split(a)
    b_high, b_low = split(b)
    dot = functools.partial(
        lax.dot_general, dimension_numbers=dims, preferred_element_type=jnp.float32
    )
    return dot(a_high, b_high) + (dot(a_high, b_low) + dot(a_low, b_high))


def wrap(value, count):
    return lax.rem(value + count, count)


def kernel(
    g_ref, o_ref, s_out, r_out,
    gi, gj, row1, col1, row2, col2, norms,
    gi_send, gi_recv, gj_send, gj_recv,
    c1_send, c1_recv, r1_send, r1_recv,
    c2_send, c2_recv, r2_send, r2_recv,
    n_send, n_recv, local_sem,
):
    i = lax.axis_index("gx")
    j = lax.axis_index("gy")
    ix = i + 1 - 2 * lax.rem(i, 2)
    jx = j + 2 - 4 * lax.rem(lax.div(j, 2), 2)
    jc = j + 1 - 2 * lax.rem(j, 2)
    pending = []

    def send(src, dst, send_sem, recv_sem, to):
        copy = pltpu.make_async_remote_copy(
            src_ref=src, dst_ref=dst, send_sem=send_sem, recv_sem=recv_sem,
            device_id=to, device_id_type=MESH,
        )
        copy.start()
        pending.append(copy)

    def arrived(dst, recv_sem, send_sem):
        pltpu.make_async_remote_copy(
            src_ref=dst, dst_ref=dst, send_sem=send_sem, recv_sem=recv_sem,
            device_id=(i, jc), device_id_type=MESH,
        ).wait_recv()

    barrier = pltpu.get_barrier_semaphore()

    def greet(to):
        pl.semaphore_signal(barrier, inc=1, device_id=to, device_id_type=MESH)

    for r in range(1, N_GY):
        greet((i, wrap(j + r, N_GY)))
    for r in range(1, N_GX):
        greet((wrap(i + r, N_GX), j))
    for r in range(1, N_GY):
        greet((j, wrap(j + r, N_GY)))

    @pl.when(i != j)
    def _():
        greet((j, j))

    mine = pl.ds(pl.multiple_of(j * PIECE, PIECE), PIECE)
    gi[mine, :] = g_ref[...].T

    @pl.when(i != j)
    def _():
        pl.semaphore_wait(barrier, 46)

    @pl.when(i == j)
    def _():
        pl.semaphore_wait(barrier, 45)

    first = pltpu.make_async_remote_copy(
        src_ref=gi.at[mine], dst_ref=gj.at[mine], send_sem=gj_send.at[0], recv_sem=gj_recv.at[j],
        device_id=(i, i), device_id_type=MESH,
    )
    here = pltpu.make_async_copy(gi.at[mine], gj.at[mine], local_sem)

    @pl.when(i != j)
    def _():
        first.start()

    @pl.when(i == j)
    def _():
        here.start()

    for r in range(1, N_GX):
        send(gi.at[mine], gj.at[mine], gj_send.at[r], gj_recv.at[j], (wrap(i + r, N_GX), i))
        send(gi.at[mine], gi.at[mine], gi_send.at[r], gi_recv.at[r], (i, wrap(j + r, N_GY)))
    for r in range(1, N_GY):
        m = wrap(j + N_GY - r, N_GY)
        part = pl.ds(pl.multiple_of(m * PIECE, PIECE), PIECE)
        arrived(gi.at[part], gi_recv.at[r], gi_send.at[r])
    for r in range(1, N_GY):
        m = wrap(j + r, N_GY)
        part = pl.ds(pl.multiple_of(m * PIECE, PIECE), PIECE)
        arrived(gj.at[part], gj_recv.at[m], gj_send.at[0])

    @pl.when(i != j)
    def _():
        arrived(gj.at[mine], gj_recv.at[j], gj_send.at[0])

    @pl.when(i == j)
    def _():
        here.wait()

    outer = dot3(gi[...], gj[...], (((0,), (0,)), ((), ())))
    stat = 0.9 * o_ref[...] + outer * (1.0 / (N_GY * PIECE))

    def gather(row, col, c_send, c_recv, r_send, r_recv):
        def col_part(slot, h):
            return col.at[slot, pl.ds(h * HALF, HALF)]

        def col_send(key, slot, h, to):
            q = COL_AT[key]
            send(col_part(slot, h), col_part(slot, h), c_send.at[q], c_recv.at[q], to)

        def col_wait(key, slot, h):
            q = COL_AT[key]
            arrived(col_part(slot, h), c_recv.at[q], c_send.at[q])

        def row_part(slot, h):
            return row.at[slot] if h is None else row.at[slot, pl.ds(h * HALF, HALF)]

        def row_send(key, slot, h, to):
            q = ROW_AT[key]
            send(row_part(slot, h), row_part(slot, h), r_send.at[q], r_recv.at[q], to)

        def row_wait(key, slot, h):
            q = ROW_AT[key]
            arrived(row_part(slot, h), r_recv.at[q], r_send.at[q])

        z_to = [(wrap(i + 2, 16), j), (wrap(i + 14, 16), j)]
        x_to = (ix, j)
        y_to = [(i, wrap(j + 4, 16)), (i, wrap(j + 12, 16))]
        h_to = (i, jx)
        c_to = (i, jc)
        z_off = [14, 2]
        y_off = [12, 4]

        def z_slot(base, d, s):
            return wrap(base + z_off[d] * s, 16)

        def y_slot(base, d, s):
            return wrap(base + y_off[d] * s, 16)

        col_send(("x", 0), i, 0, x_to)
        for d in (0, 1):
            col_send(("z", d, 0, 0, 1), i, 0, z_to[d])
        row_send(("x", 0), j, None, h_to)
        for d in (0, 1):
            row_send(("y", d, 0, 1), j, None, y_to[d])
        for d in (0, 1):
            col_send(("z", d, 0, 1, 1), i, 1, z_to[d])
        col_send(("xb", 0, 0), i, 1, x_to)
        row_send(("c", 0, 0), j, None, c_to)
        col_wait(("x", 0), ix, 0)
        for d in (0, 1):
            col_send(("z", d, 1, 0, 1), ix, 0, z_to[d])
        row_wait(("x", 0), jx, None)
        for d in (0, 1):
            row_send(("y", d, 1, 1), jx, None, y_to[d])
        row_send(("c", 1, 0), jx, None, c_to)
        for s in (1, 2, 3, 4):
            for h in (0, 1):
                for d in (0, 1):
                    if ("z", d, 0, h, s) not in COL_AT:
                        continue
                    slot = z_slot(i, d, s)
                    col_wait(("z", d, 0, h, s), slot, h)
                    if ("z", d, 0, h, s + 1) in COL_AT:
                        col_send(("z", d, 0, h, s + 1), slot, h, z_to[d])
                    if h == 1:
                        col_send(("xb", d, s), slot, h, x_to)
            for d in (0, 1):
                if ("z", d, 1, 0, s) not in COL_AT:
                    continue
                slot = z_slot(ix, d, s)
                col_wait(("z", d, 1, 0, s), slot, 0)
                if ("z", d, 1, 0, s + 1) in COL_AT:
                    col_send(("z", d, 1, 0, s + 1), slot, 0, z_to[d])
            for st, base in ((0, j), (1, jx)):
                if s == 1:
                    for d in (0, 1):
                        slot = y_slot(base, d, 1)
                        row_wait(("y", d, st, 1), slot, None)
                        row_send(("y", d, st, 2), slot, d, y_to[d])
                        row_send(("c", st, 1 + d), slot, None, c_to)
                if s == 2:
                    slot = y_slot(base, 0, 2)
                    for d in (0, 1):
                        row_wait(("y", d, st, 2), slot, d)
                    row_send(("c", st, 3), slot, None, c_to)
        for st, base in ((0, jc), (1, jx + jc - j)):
            for t, (d, s) in enumerate(((0, 0), (0, 1), (1, 1), (0, 2))):
                row_wait(("c", st, t), y_slot(base, d, s), None)
        for key in COL_KEYS:
            if key[0] == "xb":
                col_wait(key, z_slot(ix, key[1], key[2]), 1)

    row1[j] = stat
    col1[i] = stat
    s_out[...] = stat
    gather(row1, col1, c1_send, c1_recv, r1_send, r1_recv)

    squares = jnp.zeros((B, B), jnp.float32)
    for k in range(N_GY):
        squares = squares + row1[k] * row1[k]
    norms[i] = jnp.sum(squares, axis=0, keepdims=True)
    for r in range(1, N_GX):
        send(norms.at[i], norms.at[i], n_send.at[r], n_recv.at[r], (wrap(i + r, N_GX), j))

    def pair(ref, k, axis):
        return jnp.concatenate([ref[2 * k], ref[2 * k + 1]], axis=axis)

    power = jnp.zeros((B, B), jnp.float32)
    for k in range(N_GX // 2):
        power = power + dot3(pair(row1, k, 1), pair(col1, k, 0))
    row2[j] = power
    col2[i] = power
    gather(row2, col2, c2_send, c2_recv, r2_send, r2_recv)
    for r in range(1, N_GX):
        m = wrap(i + N_GX - r, N_GX)
        arrived(norms.at[m], n_recv.at[r], n_send.at[r])
    total = jnp.sum(jnp.sum(norms[...], axis=0), axis=1, keepdims=True)
    inv = 1.0 / (2.0 * jnp.sqrt(total * (1.0 / (N_GX * B))))
    inv2 = inv * inv
    c3 = -0.5625 * inv2 * inv
    c4 = 0.0625 * inv2 * inv2
    result = jnp.zeros((B, B), jnp.float32)
    for k in range(N_GX // 2):
        result = result + dot3(pair(row2, k, 1), c3 * pair(col1, k, 0) + c4 * pair(col2, k, 0))
    rows = lax.broadcasted_iota(jnp.int32, (B, B), 0)
    cols = lax.broadcasted_iota(jnp.int32, (B, B), 1)
    constant = jnp.where((rows == cols) & (i == j), 2.25, 0.0)
    r_out[...] = constant + (-2.4375 * inv) * s_out[...] + (1.6875 * inv2) * row2[j] + result

    @pl.when(i != j)
    def _():
        first.wait_send()

    for copy in pending:
        copy.wait_send()


def local(gradient, stat_old):
    dma = pltpu.SemaphoreType.DMA
    n_col, n_row = len(COL_KEYS), len(ROW_KEYS)
    block = jax.ShapeDtypeStruct((B, B), jnp.float32)
    return pl.pallas_call(
        kernel,
        out_shape=(block, block),
        in_specs=[pl.BlockSpec(memory_space=pltpu.VMEM)] * 2,
        out_specs=[pl.BlockSpec(memory_space=pltpu.VMEM)] * 2,
        scratch_shapes=[
            pltpu.VMEM((N_GY * PIECE, B), jnp.float32),
            pltpu.VMEM((N_GY * PIECE, B), jnp.float32),
            pltpu.VMEM((N_GY, B, B), jnp.float32),
            pltpu.VMEM((N_GX, B, B), jnp.float32),
            pltpu.VMEM((N_GY, B, B), jnp.float32),
            pltpu.VMEM((N_GX, B, B), jnp.float32),
            pltpu.VMEM((N_GX, 1, B), jnp.float32),
            dma((N_GX,)), dma((N_GX,)), dma((N_GX,)), dma((N_GX,)),
            dma((n_col,)), dma((n_col,)), dma((n_row,)), dma((n_row,)),
            dma((n_col,)), dma((n_col,)), dma((n_row,)), dma((n_row,)),
            dma((N_GX,)), dma((N_GX,)), dma(()),
        ],
        compiler_params=pltpu.CompilerParams(collective_id=0, has_side_effects=True),
        name="shampoo",
    )(gradient, stat_old)


def solution(mesh):
    placed = (P("gx", "gy"), P("gx", "gy"))
    return jax.shard_map(local, mesh=mesh, in_specs=placed, out_specs=placed, check_vma=False)
```

```python
import functools

import jax
import jax.numpy as jnp
from jax import lax
from jax.experimental import pallas as pl
from jax.experimental.pallas import tpu as pltpu
from jax.sharding import PartitionSpec as P

MESH = pl.DeviceIdType.MESH
N = 16
B = 128
HALF = B // 2
PIECE = 32
STEPS = (1, 3, 2)

ROW_KEYS = (
    [("x", dx, h) for dx in STEPS for h in (0, 1)]
    + [("y", dy, h) for dy in STEPS for h in (0, 1)]
    + [("xy", dx, dy) for dx in STEPS for dy in STEPS]
    + [("yx", dx, dy) for dx in STEPS for dy in STEPS]
)
COL_KEYS = (
    [("z", 2, d, h) for d in (0, 1) for h in (0, 1)]
    + [("z", 1, d) for d in (0, 1)]
    + [("z", 3, d, h) for d in (0, 1) for h in (0, 1)]
    + [("z", 4, d) for d in (0, 1)]
    + [("c", dz) for dz in range(8)]
)
ROW_AT = {key: number for number, key in enumerate(ROW_KEYS)}
COL_AT = {key: number for number, key in enumerate(COL_KEYS)}


def split(x):
    high = x.astype(jnp.bfloat16)
    low = (x - high.astype(jnp.float32)).astype(jnp.bfloat16)
    return high, low


def dot3(a, b, dims=(((1,), (0,)), ((), ()))):
    a_high, a_low = split(a)
    b_high, b_low = split(b)
    dot = functools.partial(
        lax.dot_general, dimension_numbers=dims, preferred_element_type=jnp.float32
    )
    return dot(a_high, b_high) + (dot(a_high, b_low) + dot(a_low, b_high))


def kernel(
    g_hbm, o_hbm, s_out, r_out,
    g_own, o_own, o_far, s_far, r_own, r_far,
    gi, gj, row1, col1, row2, col2, norms,
    local_sem, g_send, gi_recv, gj_recv, gc_recv,
    c_send, r_send, c1_recv, r1_recv, c2_recv, r2_recv,
    n_send, n_recv, swap_send, swap_recv,
):
    i = lax.axis_index("gx")
    j = lax.axis_index("gy")
    z, xl = lax.div(i, 2), lax.rem(i, 2)
    y, xh, c = lax.div(j, 4), lax.rem(lax.div(j, 2), 2), lax.rem(j, 2)
    x = xh * 2 + xl
    ti = z * 2 + c
    tj = y * 4 + x
    swapped = c != xl

    def at(pz, px, py, pc):
        return (pz * 2 + lax.rem(px, 2), py * 4 + lax.div(px, 2) * 2 + pc)

    def step(value, by, size):
        return lax.rem(value + by, size)

    def remote(src, dst, send_sem, recv_sem, to):
        return pltpu.make_async_remote_copy(
            src_ref=src, dst_ref=dst, send_sem=send_sem, recv_sem=recv_sem,
            device_id=to, device_id_type=MESH,
        )

    def bytes_of(ref, sem):
        pltpu.make_async_copy(ref, ref, sem).wait()

    g_in = pltpu.make_async_copy(g_hbm, g_own, local_sem.at[0])
    o_in = pltpu.make_async_copy(o_hbm, o_own, local_sem.at[1])
    g_in.start()
    o_in.start()

    barrier = pltpu.get_barrier_semaphore()

    def greet(to):
        pl.semaphore_signal(barrier, inc=1, device_id=to, device_id_type=MESH)

    for r in range(1, N):
        greet((ti, step(j, r, N)))

    @pl.when(swapped)
    def _():
        greet((ti, j))
        greet((ti, tj))

    for r in range(1, 8):
        greet((tj, step(j, 2 * r, N)))

    @pl.when(i != tj)
    def _():
        greet((tj, j))

    for s in STEPS:
        greet(at(z, step(x, s, 4), y, c))
        greet(at(z, x, step(y, s, 4), c))
    for s in range(1, 8):
        greet(at(step(z, s, 8), x, y, c))
    for s in range(8):
        greet(at(step(z, s, 8), x, y, 1 - c))
    g_in.wait()
    same = 1 - (c - xl) * (c - xl)
    pl.semaphore_wait(barrier, 46 - 2 * same - (i == tj).astype(jnp.int32))

    order = lax.rem(j, 2) * 8 + lax.div(j, 2)
    mine = pl.ds(pl.multiple_of(order * PIECE, PIECE), PIECE)
    ky, kx = lax.div(i, 4), lax.rem(i, 4)
    gi_near = remote(g_own, gi.at[mine], g_send, gi_recv, (i, y * 4 + xh * 2 + xl))
    gj_near = remote(g_own, gj.at[mine], g_send, gj_recv, at(z, kx, ky, c))
    gi_here = pltpu.make_async_copy(g_own, gi.at[mine], local_sem.at[0])
    gj_here = pltpu.make_async_copy(g_own, gj.at[mine], local_sem.at[2])

    for r in range(1, 8):
        remote(g_own, gj.at[mine], g_send, gj_recv, at(step(z, r, 8), kx, ky, c)).start()

    @pl.when(i != tj)
    def _():
        gj_near.start()

    @pl.when(i == tj)
    def _():
        gj_here.start()

    for r in range(N):
        sx, sy = r % 4, r // 4
        if r:
            remote(
                g_own, gi.at[mine], g_send, gi_recv, at(z, step(x, sx, 4), step(y, sy, 4), xl)
            ).start()

    @pl.when(swapped)
    def _():
        gi_near.start()

    @pl.when(jnp.logical_not(swapped))
    def _():
        gi_here.start()

    o_in.wait()
    o_swap = remote(o_own, o_far, swap_send.at[0], swap_recv.at[0], (ti, tj))

    @pl.when(swapped)
    def _():
        o_swap.start()

    quarter = 8 * PIECE

    @pl.when(i != tj)
    def _():
        bytes_of(gj.at[pl.ds(0, quarter)], gj_recv)

    @pl.when(i == tj)
    def _():
        bytes_of(gj.at[pl.ds(0, quarter - PIECE)], gj_recv)
        gj_here.wait()

    mine_half = pl.ds(pl.multiple_of(c * quarter, quarter), quarter)
    other_half = pl.ds(pl.multiple_of((1 - c) * quarter, quarter), quarter)
    gj_share = remote(gj.at[mine_half], gj.at[mine_half], g_send, gc_recv, (i, j + 1 - 2 * c))
    gj_share.start()

    @pl.when(swapped)
    def _():
        bytes_of(gi, gi_recv)

    @pl.when(jnp.logical_not(swapped))
    def _():
        bytes_of(gi.at[pl.ds(0, 15 * PIECE)], gi_recv)
        gi_here.wait()

    remote(
        gj.at[other_half], gj.at[other_half], g_send, gc_recv, (i, j + 1 - 2 * c)
    ).wait_recv()

    outer = dot3(gi[...], gj[...], (((0,), (0,)), ((), ())))

    @pl.when(swapped)
    def _():
        o_swap.wait_send()
        o_swap.wait_recv()
        o_own[...] = o_far[...]

    stat = 0.9 * o_own[...] + outer * (1.0 / (N * PIECE))

    def gather(row, col, c_send, c_recv, r_send, r_recv):
        def row_part(slot, h):
            return row.at[slot, pl.ds(h * HALF, HALF)]

        def row_send(key, slot, h, to):
            part = row_part(slot, h)
            remote(part, part, r_send, r_recv.at[ROW_AT[key]], to).start()

        def row_wait(key, slot, h):
            part = row_part(slot, h)
            remote(part, part, r_send, r_recv.at[ROW_AT[key]], (i, j + 1 - 2 * c)).wait_recv()

        def col_part(slot, h):
            return col.at[slot] if h is None else col.at[slot, pl.ds(h * HALF, HALF)]

        def col_send(key, slot, h, to):
            part = col_part(slot, h)
            remote(part, part, c_send, c_recv.at[COL_AT[key]], to).start()

        def col_wait(key, slot, h):
            part = col_part(slot, h)
            remote(part, part, c_send, c_recv.at[COL_AT[key]], (i, j + 1 - 2 * c)).wait_recv()

        def x_to(s):
            return at(z, step(x, s, 4), y, c)

        def y_to(s):
            return at(z, x, step(y, s, 4), c)

        def z_to(s):
            return at(step(z, s, 8), x, y, c)

        def from_xy(dx, dy):
            return step(y, 4 - dy, 4) * 4 + step(x, 4 - dx, 4)

        def from_z(dz, core):
            return step(z, 8 - dz, 8) * 2 + core

        other = (i, j + 1 - 2 * c)
        away = (2, 6)
        near = (1, 7)
        for h in (0, 1):
            for d in (0, 1):
                col_send(("z", 2, d, h), ti, h, z_to(away[d]))
            for s in STEPS:
                row_send(("x", s, h), tj, h, x_to(s))
                row_send(("y", s, 1 - h), tj, 1 - h, y_to(s))
        for d in (0, 1):
            col_send(("z", 1, d), ti, None, z_to(near[d]))
        col_send(("c", 0), ti, None, other)

        for s in STEPS:
            row_wait(("x", s, 0), from_xy(s, 0), 0)
            for t in STEPS:
                row_send(("xy", s, t), from_xy(s, 0), 0, y_to(t))
            row_wait(("y", s, 1), from_xy(0, s), 1)
            for t in STEPS:
                row_send(("yx", t, s), from_xy(0, s), 1, x_to(t))
        for h in (0, 1):
            for d in (0, 1):
                slot = from_z(away[d], c)
                col_wait(("z", 2, d, h), slot, h)
                if h == d:
                    col_send(("z", 4, d), slot, h, z_to(away[d]))
                col_send(("z", 3, d, h), slot, h, z_to(near[d]))
        for d in (0, 1):
            col_send(("c", away[d]), from_z(away[d], c), None, other)
        for d in (0, 1):
            col_wait(("z", 1, d), from_z(near[d], c), None)
            col_send(("c", near[d]), from_z(near[d], c), None, other)
        for d in (0, 1):
            slot = from_z((away[d] + near[d]) % 8, c)
            for h in (0, 1):
                col_wait(("z", 3, d, h), slot, h)
            col_send(("c", (away[d] + near[d]) % 8), slot, None, other)
        for d in (0, 1):
            col_wait(("z", 4, d), from_z(4, c), d)
        col_send(("c", 4), from_z(4, c), None, other)
        for s in STEPS:
            row_wait(("x", s, 1), from_xy(s, 0), 1)
            row_wait(("y", s, 0), from_xy(0, s), 0)
        for s in STEPS:
            for t in STEPS:
                row_wait(("xy", s, t), from_xy(s, t), 0)
                row_wait(("yx", t, s), from_xy(t, s), 1)
        for dz in range(8):
            col_wait(("c", dz), from_z(dz, 1 - c), None)

    row1[tj] = stat
    col1[ti] = stat
    s_out[...] = stat
    gather(row1, col1, c_send.at[0], c1_recv, r_send.at[0], r1_recv)
    s_swap = remote(row1.at[tj], s_far, swap_send.at[1], swap_recv.at[1], (ti, tj))

    @pl.when(swapped)
    def _():
        s_swap.start()

    squares = jnp.zeros((B, B), jnp.float32)
    for k in range(N):
        squares = squares + row1[k] * row1[k]
    norms[ti] = jnp.sum(squares, axis=0, keepdims=True)
    for r in range(1, N):
        remote(
            norms.at[ti], norms.at[ti], n_send, n_recv,
            at(step(z, r // 2, 8), x, y, step(c, r % 2, 2)),
        ).start()

    def pair(ref, k, axis):
        return jnp.concatenate([ref[2 * k], ref[2 * k + 1]], axis=axis)

    power = jnp.zeros((B, B), jnp.float32)
    for k in range(N // 2):
        power = power + dot3(pair(row1, k, 1), pair(col1, k, 0))
    row2[tj] = power
    col2[ti] = power
    gather(row2, col2, c_send.at[1], c2_recv, r_send.at[1], r2_recv)
    bytes_of(norms.at[pl.ds(0, N - 1)], n_recv)
    total = jnp.sum(jnp.sum(norms[...], axis=0), axis=1, keepdims=True)
    inv = 1.0 / (2.0 * jnp.sqrt(total * (1.0 / (N * B))))
    inv2 = inv * inv
    c3 = -0.5625 * inv2 * inv
    c4 = 0.0625 * inv2 * inv2
    result = jnp.zeros((B, B), jnp.float32)
    for k in range(N // 2):
        result = result + dot3(pair(row2, k, 1), c3 * pair(col1, k, 0) + c4 * pair(col2, k, 0))
    rows = lax.broadcasted_iota(jnp.int32, (B, B), 0)
    cols = lax.broadcasted_iota(jnp.int32, (B, B), 1)
    constant = jnp.where((rows == cols) & (ti == tj), 2.25, 0.0)
    result = constant + (-2.4375 * inv) * row1[tj] + (1.6875 * inv2) * row2[tj] + result
    r_own[...] = result
    r_out[...] = result
    r_swap = remote(r_own, r_far, swap_send.at[2], swap_recv.at[2], (ti, tj))

    @pl.when(swapped)
    def _():
        r_swap.start()
        s_swap.wait_send()
        s_swap.wait_recv()
        s_out[...] = s_far[...]

    for phase, (row, col) in enumerate(((row1, col1), (row2, col2))):
        bytes_of(row.at[pl.ds(0, 15)], r_send.at[phase])
        bytes_of(col.at[pl.ds(0, 15)], c_send.at[phase])
    bytes_of(norms.at[pl.ds(0, N - 1)], n_send)
    bytes_of(gj.at[pl.ds(0, quarter)], g_send)
    bytes_of(gi.at[pl.ds(0, 22 * PIECE - 8 * PIECE)], g_send)
    bytes_of(gj.at[pl.ds(0, 8 * PIECE)], g_send)

    @pl.when(swapped)
    def _():
        bytes_of(g_own, g_send)

    @pl.when(i != tj)
    def _():
        bytes_of(g_own, g_send)

    @pl.when(swapped)
    def _():
        r_swap.wait_send()
        r_swap.wait_recv()
        r_out[...] = r_far[...]


def local(gradient, stat_old):
    dma = pltpu.SemaphoreType.DMA
    n_col, n_row = len(COL_KEYS), len(ROW_KEYS)
    block = jax.ShapeDtypeStruct((B, B), jnp.float32)
    tile = pltpu.VMEM((B, B), jnp.float32)
    panel = pltpu.VMEM((N, B, B), jnp.float32)
    pieces = pltpu.VMEM((N * PIECE, B), jnp.float32)
    return pl.pallas_call(
        kernel,
        out_shape=(block, block),
        in_specs=[pl.BlockSpec(memory_space=pltpu.HBM)] * 2,
        out_specs=[pl.BlockSpec(memory_space=pltpu.VMEM)] * 2,
        scratch_shapes=[
            pltpu.VMEM((PIECE, B), jnp.float32), tile, tile, tile, tile, tile,
            pieces, pieces, panel, panel, panel, panel, pltpu.VMEM((N, 1, B), jnp.float32),
            dma((3,)), dma(()), dma(()), dma(()), dma(()),
            dma((2,)), dma((2,)), dma((n_col,)), dma((n_row,)), dma((n_col,)), dma((n_row,)),
            dma(()), dma(()), dma((3,)), dma((3,)),
        ],
        compiler_params=pltpu.CompilerParams(
            collective_id=0, has_side_effects=True, vmem_limit_bytes=16 * 1024 * 1024
        ),
        name="shampoo",
    )(gradient.T, stat_old)


def solution(mesh):
    placed = (P("gx", "gy"), P("gx", "gy"))
    return jax.shard_map(local, mesh=mesh, in_specs=placed, out_specs=placed, check_vma=False)
```

```python
import functools

import jax
import jax.numpy as jnp
from jax import lax
from jax.experimental import pallas as pl
from jax.experimental.pallas import tpu as pltpu
from jax.sharding import PartitionSpec as P

MESH = pl.DeviceIdType.MESH
N = 16
B = 128
HALF = B // 2
PIECE = 32
STEPS = (1, 3, 2)

ROW_KEYS = [("x", s) for s in STEPS] + [("y", s) for s in STEPS] + ["rest"]
COL_KEYS = (
    [("z", 2, d, h) for d in (0, 1) for h in (0, 1)]
    + [("z", 1), ("z", 3, 0), ("z", 3, 1), ("z", 4), "near", "far"]
)
ROW_AT = {key: number for number, key in enumerate(ROW_KEYS)}
COL_AT = {key: number for number, key in enumerate(COL_KEYS)}


def split(x):
    high = x.astype(jnp.bfloat16)
    low = (x - high.astype(jnp.float32)).astype(jnp.bfloat16)
    return high, low


def dot3(a, b, dims=(((1,), (0,)), ((), ()))):
    a_high, a_low = split(a)
    b_high, b_low = split(b)
    dot = functools.partial(
        lax.dot_general, dimension_numbers=dims, preferred_element_type=jnp.float32
    )
    return dot(a_high, b_high) + (dot(a_high, b_low) + dot(a_low, b_high))


def kernel(
    g_hbm, o_hbm, s_out, r_out,
    g_own, o_own, o_far, s_far, r_own, r_far,
    gi, gj, row1, col1, row2, col2, norms,
    local_sem, g_send, gi_recv, gj_recv, gc_recv,
    c_send, r_send, c1_recv, r1_recv, c2_recv, r2_recv,
    n_send, n_recv, swap_send, swap_recv,
):
    i = lax.axis_index("gx")
    j = lax.axis_index("gy")
    z, xl = lax.div(i, 2), lax.rem(i, 2)
    y, xh, c = lax.div(j, 4), lax.rem(lax.div(j, 2), 2), lax.rem(j, 2)
    x = xh * 2 + xl
    ti = z * 2 + c
    tj = y * 4 + x
    swapped = c != xl

    def at(pz, px, py, pc):
        return (pz * 2 + lax.rem(px, 2), py * 4 + lax.div(px, 2) * 2 + pc)

    def step(value, by, size):
        return lax.rem(value + by, size)

    def remote(src, dst, send_sem, recv_sem, to):
        return pltpu.make_async_remote_copy(
            src_ref=src, dst_ref=dst, send_sem=send_sem, recv_sem=recv_sem,
            device_id=to, device_id_type=MESH,
        )

    def bytes_of(ref, sem):
        pltpu.make_async_copy(ref, ref, sem).wait()

    g_in = pltpu.make_async_copy(g_hbm, g_own, local_sem.at[0])
    o_in = pltpu.make_async_copy(o_hbm, o_own, local_sem.at[1])
    g_in.start()
    o_in.start()

    barrier = pltpu.get_barrier_semaphore()

    def greet(to):
        pl.semaphore_signal(barrier, inc=1, device_id=to, device_id_type=MESH)

    for r in range(1, 8):
        greet((tj, step(j, 2 * r, N)))

    @pl.when(i != tj)
    def _():
        greet((tj, j))

    for r in range(1, N):
        greet((ti, step(j, r, N)))

    @pl.when(swapped)
    def _():
        greet((ti, j))
        greet((ti, tj))

    for s in STEPS:
        greet(at(z, step(x, s, 4), y, c))
        greet(at(z, x, step(y, s, 4), c))
    for s in range(1, 8):
        greet(at(step(z, s, 8), x, y, c))
    for s in range(8):
        greet(at(step(z, s, 8), x, y, 1 - c))
    g_in.wait()
    same = 1 - (c - xl) * (c - xl)
    pl.semaphore_wait(barrier, 46 - 2 * same - (i == tj).astype(jnp.int32))

    order = lax.rem(j, 2) * 8 + lax.div(j, 2)
    mine = pl.ds(pl.multiple_of(order * PIECE, PIECE), PIECE)
    ky, kx = lax.div(i, 4), lax.rem(i, 4)
    gi_near = remote(g_own, gi.at[mine], g_send, gi_recv, (i, y * 4 + xh * 2 + xl))
    gj_near = remote(g_own, gj.at[mine], g_send, gj_recv, at(z, kx, ky, c))
    gi_here = pltpu.make_async_copy(g_own, gi.at[mine], local_sem.at[0])
    gj_here = pltpu.make_async_copy(g_own, gj.at[mine], local_sem.at[2])

    for r in range(1, 8):
        remote(g_own, gj.at[mine], g_send, gj_recv, at(step(z, r, 8), kx, ky, c)).start()

    @pl.when(i != tj)
    def _():
        gj_near.start()

    @pl.when(i == tj)
    def _():
        gj_here.start()

    for r in range(N):
        sx, sy = r % 4, r // 4
        if r:
            remote(
                g_own, gi.at[mine], g_send, gi_recv, at(z, step(x, sx, 4), step(y, sy, 4), xl)
            ).start()

    @pl.when(swapped)
    def _():
        gi_near.start()

    @pl.when(jnp.logical_not(swapped))
    def _():
        gi_here.start()

    o_in.wait()
    o_swap = remote(o_own, o_far, swap_send.at[0], swap_recv.at[0], (ti, tj))

    @pl.when(swapped)
    def _():
        o_swap.start()

    quarter = 8 * PIECE

    @pl.when(i != tj)
    def _():
        bytes_of(gj.at[pl.ds(0, quarter)], gj_recv)

    @pl.when(i == tj)
    def _():
        bytes_of(gj.at[pl.ds(0, quarter - PIECE)], gj_recv)
        gj_here.wait()

    mine_half = pl.ds(pl.multiple_of(c * quarter, quarter), quarter)
    other_half = pl.ds(pl.multiple_of((1 - c) * quarter, quarter), quarter)
    gj_share = remote(gj.at[mine_half], gj.at[mine_half], g_send, gc_recv, (i, j + 1 - 2 * c))
    gj_share.start()

    @pl.when(swapped)
    def _():
        bytes_of(gi, gi_recv)

    @pl.when(jnp.logical_not(swapped))
    def _():
        bytes_of(gi.at[pl.ds(0, 15 * PIECE)], gi_recv)
        gi_here.wait()

    remote(
        gj.at[other_half], gj.at[other_half], g_send, gc_recv, (i, j + 1 - 2 * c)
    ).wait_recv()

    outer = dot3(gi[...], gj[...], (((0,), (0,)), ((), ())))

    @pl.when(swapped)
    def _():
        o_swap.wait_send()
        o_swap.wait_recv()
        o_own[...] = o_far[...]

    stat = 0.9 * o_own[...] + outer * (1.0 / (N * PIECE))

    def gather(row, col, c_send, c_recv, r_send, r_recv, between, product):
        def row_send(key, slot, h, to):
            part = row.at[slot, pl.ds(h * HALF, HALF)]
            remote(part, part, r_send, r_recv.at[ROW_AT[key]], to).start()

        def row_wait(key, tiles):
            bytes_of(tiles, r_recv.at[ROW_AT[key]])

        def col_part(slot, h):
            return col.at[slot] if h is None else col.at[slot, pl.ds(h * HALF, HALF)]

        def col_send(key, slot, h, to):
            part = col_part(slot, h)
            remote(part, part, c_send, c_recv.at[COL_AT[key]], to).start()

        def col_wait(key, tiles):
            bytes_of(tiles, c_recv.at[COL_AT[key]])

        def x_to(s):
            return at(z, step(x, s, 4), y, c)

        def y_to(s):
            return at(z, x, step(y, s, 4), c)

        def z_to(s):
            return at(step(z, s, 8), x, y, c)

        def from_xy(dx, dy):
            return step(y, 4 - dy, 4) * 4 + step(x, 4 - dx, 4)

        def from_z(dz, core):
            return step(z, 8 - dz, 8) * 2 + core

        other = (i, j + 1 - 2 * c)
        away = (2, 6)
        near = (1, 7)
        for h in (0, 1):
            for d in (0, 1):
                col_send(("z", 2, d, h), ti, h, z_to(away[d]))
            for s in STEPS:
                row_send(("x", s) if h == 0 else "rest", tj, h, x_to(s))
                row_send(("y", s) if h == 0 else "rest", tj, 1 - h, y_to(s))
        for d in (0, 1):
            col_send(("z", 1), ti, None, z_to(near[d]))
        col_send("near", ti, None, other)
        between()

        half = row.at[0, pl.ds(0, HALF)]
        for s in STEPS:
            row_wait(("x", s), half)
            for t in STEPS:
                row_send("rest", from_xy(s, 0), 0, y_to(t))
            row_wait(("y", s), half)
            for t in STEPS:
                row_send("rest", from_xy(0, s), 1, x_to(t))
        for h in (0, 1):
            for d in (0, 1):
                slot = from_z(away[d], c)
                col_wait(("z", 2, d, h), half)
                if h == d:
                    col_send(("z", 4), slot, h, z_to(away[d]))
                col_send(("z", 3, d), slot, h, z_to(near[d]))
        for d in (0, 1):
            col_send("near", from_z(away[d], c), None, other)
        col_wait(("z", 1), col.at[pl.ds(0, 2)])
        for d in (0, 1):
            col_send("near", from_z(near[d], c), None, other)
        for d in (0, 1):
            col_wait(("z", 3, d), col.at[0])
            col_send("far", from_z((away[d] + near[d]) % 8, c), None, other)
        col_wait(("z", 4), col.at[0])
        col_send("far", from_z(4, c), None, other)
        row_wait("rest", row.at[pl.ds(0, 12)])
        col_wait("near", col.at[pl.ds(0, 5)])
        total = product(step(z, 0, 8))
        for dz in (1, 7, 2, 6):
            total = total + product(step(z, dz, 8))
        col_wait("far", col.at[pl.ds(0, 3)])
        for dz in (3, 5, 4):
            total = total + product(step(z, dz, 8))
        return total

    row1[tj] = stat
    col1[ti] = stat
    s_swap = remote(row1.at[tj], s_far, swap_send.at[1], swap_recv.at[1], (ti, tj))

    def pair(ref, k, axis):
        return jnp.concatenate([ref[2 * k], ref[2 * k + 1]], axis=axis)

    def keep_stat():
        s_out[...] = stat

        @pl.when(swapped)
        def _():
            s_swap.start()

    def square(k):
        return dot3(pair(row1, k, 1), pair(col1, k, 0))

    power = gather(
        row1, col1, c_send.at[0], c1_recv, r_send.at[0], r1_recv, keep_stat, square
    )
    row2[tj] = power
    col2[ti] = power

    def send_norms():
        squares = jnp.zeros((B, B), jnp.float32)
        for k in range(N):
            squares = squares + row1[k] * row1[k]
        norms[ti] = jnp.sum(squares, axis=0, keepdims=True)
        for r in range(1, N):
            remote(
                norms.at[ti], norms.at[ti], n_send, n_recv,
                at(step(z, r // 2, 8), x, y, step(c, r % 2, 2)),
            ).start()

    scales = []

    def last(k):
        if not scales:
            bytes_of(norms.at[pl.ds(0, N - 1)], n_recv)
            total = jnp.sum(jnp.sum(norms[...], axis=0), axis=1, keepdims=True)
            inv = 1.0 / (2.0 * jnp.sqrt(total * (1.0 / (N * B))))
            scales.extend((inv, inv * inv))
        inv, inv2 = scales
        factor = (-0.5625 * inv2 * inv) * pair(col1, k, 0) + (0.0625 * inv2 * inv2) * pair(col2, k, 0)
        return dot3(pair(row2, k, 1), factor)

    result = gather(
        row2, col2, c_send.at[1], c2_recv, r_send.at[1], r2_recv, send_norms, last
    )
    inv, inv2 = scales
    rows = lax.broadcasted_iota(jnp.int32, (B, B), 0)
    cols = lax.broadcasted_iota(jnp.int32, (B, B), 1)
    constant = jnp.where((rows == cols) & (ti == tj), 2.25, 0.0)
    result = constant + (-2.4375 * inv) * row1[tj] + (1.6875 * inv2) * row2[tj] + result
    r_own[...] = result
    r_out[...] = result
    r_swap = remote(r_own, r_far, swap_send.at[2], swap_recv.at[2], (ti, tj))

    @pl.when(swapped)
    def _():
        r_swap.start()
        s_swap.wait_send()
        s_swap.wait_recv()
        s_out[...] = s_far[...]

    for phase, (row, col) in enumerate(((row1, col1), (row2, col2))):
        bytes_of(row.at[pl.ds(0, 15)], r_send.at[phase])
        bytes_of(col.at[pl.ds(0, 15)], c_send.at[phase])
    bytes_of(norms.at[pl.ds(0, N - 1)], n_send)
    bytes_of(gj.at[pl.ds(0, quarter)], g_send)
    bytes_of(gi.at[pl.ds(0, 22 * PIECE - 8 * PIECE)], g_send)
    bytes_of(gj.at[pl.ds(0, 8 * PIECE)], g_send)

    @pl.when(swapped)
    def _():
        bytes_of(g_own, g_send)

    @pl.when(i != tj)
    def _():
        bytes_of(g_own, g_send)

    @pl.when(swapped)
    def _():
        r_swap.wait_send()
        r_swap.wait_recv()
        r_out[...] = r_far[...]


def store(s_ref, r_ref, s_hbm, r_hbm, sems):
    copies = [
        pltpu.make_async_copy(s_ref, s_hbm, sems.at[0]),
        pltpu.make_async_copy(r_ref, r_hbm, sems.at[1]),
    ]
    for copy in copies:
        copy.start()
    for copy in copies:
        copy.wait()


def local(gradient, stat_old):
    dma = pltpu.SemaphoreType.DMA
    n_col, n_row = len(COL_KEYS), len(ROW_KEYS)
    block = jax.ShapeDtypeStruct((B, B), jnp.float32)
    tile = pltpu.VMEM((B, B), jnp.float32)
    panel = pltpu.VMEM((N, B, B), jnp.float32)
    pieces = pltpu.VMEM((N * PIECE, B), jnp.float32)
    made = pl.pallas_call(
        kernel,
        out_shape=(block, block),
        in_specs=[pl.BlockSpec(memory_space=pltpu.HBM)] * 2,
        out_specs=[pl.BlockSpec(memory_space=pltpu.VMEM)] * 2,
        scratch_shapes=[
            pltpu.VMEM((PIECE, B), jnp.float32), tile, tile, tile, tile, tile,
            pieces, pieces, panel, panel, panel, panel, pltpu.VMEM((N, 1, B), jnp.float32),
            dma((3,)), dma(()), dma(()), dma(()), dma(()),
            dma((2,)), dma((2,)), dma((n_col,)), dma((n_row,)), dma((n_col,)), dma((n_row,)),
            dma(()), dma(()), dma((3,)), dma((3,)),
        ],
        compiler_params=pltpu.CompilerParams(
            collective_id=0, has_side_effects=True, vmem_limit_bytes=16 * 1024 * 1024
        ),
        name="shampoo",
    )(
        pltpu.with_memory_space_constraint(gradient.T, pltpu.HBM),
        pltpu.with_memory_space_constraint(stat_old, pltpu.HBM),
    )
    return pl.pallas_call(
        store,
        out_shape=(block, block),
        in_specs=[pl.BlockSpec(memory_space=pltpu.VMEM)] * 2,
        out_specs=[pl.BlockSpec(memory_space=pltpu.HBM)] * 2,
        scratch_shapes=[dma((2,))],
        compiler_params=pltpu.CompilerParams(vmem_limit_bytes=1024 * 1024),
        name="store",
    )(*made)


def solution(mesh):
    placed = (P("gx", "gy"), P("gx", "gy"))
    return jax.shard_map(local, mesh=mesh, in_specs=placed, out_specs=placed, check_vma=False)
```

```python
import functools

import jax
import jax.numpy as jnp
from jax import lax
from jax.experimental import pallas as pl
from jax.experimental.pallas import tpu as pltpu
from jax.sharding import PartitionSpec as P

MESH = pl.DeviceIdType.MESH
N = 16
B = 128
HALF = B // 2
PIECE = 32
STEPS = (1, 3, 2)

ROW_KEYS = [("x", s) for s in STEPS] + [("y", s) for s in STEPS] + ["rest"]
COL_KEYS = (
    [("z", 2, d, h) for d in (0, 1) for h in (0, 1)]
    + [("z", 1), ("z", 3, 0), ("z", 3, 1), ("z", 4), "near", "far"]
)
ROW_AT = {key: number for number, key in enumerate(ROW_KEYS)}
COL_AT = {key: number for number, key in enumerate(COL_KEYS)}


def split(x):
    high = x.astype(jnp.bfloat16)
    low = (x - high.astype(jnp.float32)).astype(jnp.bfloat16)
    return high, low


def dot3(a, b, dims=(((1,), (0,)), ((), ()))):
    a_high, a_low = split(a)
    b_high, b_low = split(b)
    dot = functools.partial(
        lax.dot_general, dimension_numbers=dims, preferred_element_type=jnp.float32
    )
    return dot(a_high, b_high) + (dot(a_high, b_low) + dot(a_low, b_high))


def kernel(
    g_hbm, o_hbm, s_out, r_out,
    g_own, o_own, o_far, s_far, r_own, r_far,
    gi, gj, row1, col1, row2, col2, norms,
    local_sem, g_send, gi_recv, gj_recv, gc_recv,
    c_send, r_send, c1_recv, r1_recv, c2_recv, r2_recv,
    n_send, n_recv, swap_send, swap_recv,
):
    i = lax.axis_index("gx")
    j = lax.axis_index("gy")
    z, xl = lax.div(i, 2), lax.rem(i, 2)
    y, xh, c = lax.div(j, 4), lax.rem(lax.div(j, 2), 2), lax.rem(j, 2)
    x = xh * 2 + xl
    ti = z * 2 + c
    tj = y * 4 + x
    swapped = c != xl

    def at(pz, px, py, pc):
        return (pz * 2 + lax.rem(px, 2), py * 4 + lax.div(px, 2) * 2 + pc)

    def step(value, by, size):
        return lax.rem(value + by, size)

    def remote(src, dst, send_sem, recv_sem, to):
        return pltpu.make_async_remote_copy(
            src_ref=src, dst_ref=dst, send_sem=send_sem, recv_sem=recv_sem,
            device_id=to, device_id_type=MESH,
        )

    def bytes_of(ref, sem):
        pltpu.make_async_copy(ref, ref, sem).wait()

    g_in = pltpu.make_async_copy(g_hbm, g_own, local_sem.at[0])
    o_in = pltpu.make_async_copy(o_hbm, o_own, local_sem.at[1])
    g_in.start()
    o_in.start()

    barrier = pltpu.get_barrier_semaphore()

    def greet(to):
        pl.semaphore_signal(barrier, inc=1, device_id=to, device_id_type=MESH)

    for r in range(1, 8):
        greet((tj, step(j, 2 * r, N)))

    @pl.when(i != tj)
    def _():
        greet((tj, j))

    for r in range(1, N):
        greet((ti, step(j, r, N)))

    @pl.when(swapped)
    def _():
        greet((ti, j))
        greet((ti, tj))

    for s in STEPS:
        greet(at(z, step(x, s, 4), y, c))
        greet(at(z, x, step(y, s, 4), c))
    for s in range(1, 8):
        greet(at(step(z, s, 8), x, y, c))
    for s in range(8):
        greet(at(step(z, s, 8), x, y, 1 - c))
    g_in.wait()
    same = 1 - (c - xl) * (c - xl)
    pl.semaphore_wait(barrier, 46 - 2 * same - (i == tj).astype(jnp.int32))

    order = lax.rem(j, 2) * 8 + lax.div(j, 2)
    mine = pl.ds(pl.multiple_of(order * PIECE, PIECE), PIECE)
    ky, kx = lax.div(i, 4), lax.rem(i, 4)
    gi_near = remote(g_own, gi.at[mine], g_send, gi_recv, (i, y * 4 + xh * 2 + xl))
    gj_near = remote(g_own, gj.at[mine], g_send, gj_recv, at(z, kx, ky, c))
    gi_here = pltpu.make_async_copy(g_own, gi.at[mine], local_sem.at[0])
    gj_here = pltpu.make_async_copy(g_own, gj.at[mine], local_sem.at[2])

    for r in (4, 3, 5, 2, 6, 1, 7):
        remote(g_own, gj.at[mine], g_send, gj_recv, at(step(z, r, 8), kx, ky, c)).start()

    @pl.when(i != tj)
    def _():
        gj_near.start()

    @pl.when(i == tj)
    def _():
        gj_here.start()

    for r in (10, 2, 8, 6, 14, 9, 11, 5, 7, 13, 15, 1, 3, 4, 12, 0):
        sx, sy = r % 4, r // 4
        if r:
            remote(
                g_own, gi.at[mine], g_send, gi_recv, at(z, step(x, sx, 4), step(y, sy, 4), xl)
            ).start()

    @pl.when(swapped)
    def _():
        gi_near.start()

    @pl.when(jnp.logical_not(swapped))
    def _():
        gi_here.start()

    o_in.wait()
    o_swap = remote(o_own, o_far, swap_send.at[0], swap_recv.at[0], (ti, tj))

    @pl.when(swapped)
    def _():
        o_swap.start()

    quarter = 8 * PIECE

    @pl.when(i != tj)
    def _():
        bytes_of(gj.at[pl.ds(0, quarter)], gj_recv)

    @pl.when(i == tj)
    def _():
        bytes_of(gj.at[pl.ds(0, quarter - PIECE)], gj_recv)
        gj_here.wait()

    mine_half = pl.ds(pl.multiple_of(c * quarter, quarter), quarter)
    other_half = pl.ds(pl.multiple_of((1 - c) * quarter, quarter), quarter)
    gj_share = remote(gj.at[mine_half], gj.at[mine_half], g_send, gc_recv, (i, j + 1 - 2 * c))
    gj_share.start()

    @pl.when(swapped)
    def _():
        bytes_of(gi, gi_recv)

    @pl.when(jnp.logical_not(swapped))
    def _():
        bytes_of(gi.at[pl.ds(0, 15 * PIECE)], gi_recv)
        gi_here.wait()

    remote(
        gj.at[other_half], gj.at[other_half], g_send, gc_recv, (i, j + 1 - 2 * c)
    ).wait_recv()

    outer = dot3(gi[...], gj[...], (((0,), (0,)), ((), ())))

    @pl.when(swapped)
    def _():
        o_swap.wait_send()
        o_swap.wait_recv()
        o_own[...] = o_far[...]

    stat = 0.9 * o_own[...] + outer * (1.0 / (N * PIECE))

    def gather(row, col, c_send, c_recv, r_send, r_recv, between, product):
        def row_send(key, slot, h, to):
            part = row.at[slot, pl.ds(h * HALF, HALF)]
            remote(part, part, r_send, r_recv.at[ROW_AT[key]], to).start()

        def row_wait(key, tiles):
            bytes_of(tiles, r_recv.at[ROW_AT[key]])

        def col_part(slot, h):
            return col.at[slot] if h is None else col.at[slot, pl.ds(h * HALF, HALF)]

        def col_send(key, slot, h, to):
            part = col_part(slot, h)
            remote(part, part, c_send, c_recv.at[COL_AT[key]], to).start()

        def col_wait(key, tiles):
            bytes_of(tiles, c_recv.at[COL_AT[key]])

        def x_to(s):
            return at(z, step(x, s, 4), y, c)

        def y_to(s):
            return at(z, x, step(y, s, 4), c)

        def z_to(s):
            return at(step(z, s, 8), x, y, c)

        def from_xy(dx, dy):
            return step(y, 4 - dy, 4) * 4 + step(x, 4 - dx, 4)

        def from_z(dz, core):
            return step(z, 8 - dz, 8) * 2 + core

        other = (i, j + 1 - 2 * c)
        away = (2, 6)
        near = (1, 7)
        for h in (0, 1):
            for d in (0, 1):
                col_send(("z", 2, d, h), ti, h, z_to(away[d]))
            for s in STEPS:
                row_send(("x", s) if h == 0 else "rest", tj, h, x_to(s))
                row_send(("y", s) if h == 0 else "rest", tj, 1 - h, y_to(s))
        for d in (0, 1):
            col_send(("z", 1), ti, None, z_to(near[d]))
        col_send("near", ti, None, other)
        between()

        half = row.at[0, pl.ds(0, HALF)]
        def relay_xy(s):
            row_wait(("x", s), half)
            for t in (2, 1, 3):
                row_send("rest", from_xy(s, 0), 0, y_to(t))
            row_wait(("y", s), half)
            for t in (2, 1, 3):
                row_send("rest", from_xy(0, s), 1, x_to(t))

        def relay_z(h):
            for d in (0, 1):
                slot = from_z(away[d], c)
                col_wait(("z", 2, d, h), half)
                if h == d:
                    col_send(("z", 4), slot, h, z_to(away[d]))
                col_send(("z", 3, d), slot, h, z_to(near[d]))

        relay_xy(STEPS[0])
        relay_xy(STEPS[1])
        relay_z(0)
        relay_xy(STEPS[2])
        relay_z(1)
        for d in (0, 1):
            col_send("near", from_z(away[d], c), None, other)
        col_wait(("z", 1), col.at[pl.ds(0, 2)])
        for d in (0, 1):
            col_send("near", from_z(near[d], c), None, other)
        for d in (0, 1):
            col_wait(("z", 3, d), col.at[0])
            col_send("far", from_z((away[d] + near[d]) % 8, c), None, other)
        col_wait(("z", 4), col.at[0])
        col_send("far", from_z(4, c), None, other)
        row_wait("rest", row.at[pl.ds(0, 12)])
        col_wait("near", col.at[pl.ds(0, 5)])
        total = product([step(z, dz, 8) for dz in (0, 1, 7, 2, 6)])
        col_wait("far", col.at[pl.ds(0, 3)])
        return total + product([step(z, dz, 8) for dz in (3, 5, 4)])

    row1[tj] = stat
    col1[ti] = stat
    s_swap = remote(row1.at[tj], s_far, swap_send.at[1], swap_recv.at[1], (ti, tj))

    def tiles(ref, pairs, axis):
        return jnp.concatenate([ref[2 * k + h] for k in pairs for h in (0, 1)], axis=axis)

    def keep_stat():
        s_out[...] = stat

        @pl.when(swapped)
        def _():
            s_swap.start()

    def square(pairs):
        return dot3(tiles(row1, pairs, 1), tiles(col1, pairs, 0))

    power = gather(
        row1, col1, c_send.at[0], c1_recv, r_send.at[0], r1_recv, keep_stat, square
    )
    row2[tj] = power
    col2[ti] = power

    def send_norms():
        squares = jnp.zeros((B, B), jnp.float32)
        for k in range(N):
            squares = squares + row1[k] * row1[k]
        norms[ti] = jnp.sum(squares, axis=0, keepdims=True)
        for r in range(1, N):
            remote(
                norms.at[ti], norms.at[ti], n_send, n_recv,
                at(step(z, r // 2, 8), x, y, step(c, r % 2, 2)),
            ).start()

    scales = []

    def last(pairs):
        if not scales:
            bytes_of(norms.at[pl.ds(0, N - 1)], n_recv)
            total = jnp.sum(jnp.sum(norms[...], axis=0), axis=1, keepdims=True)
            inv = 1.0 / (2.0 * jnp.sqrt(total * (1.0 / (N * B))))
            scales.extend((inv, inv * inv))
        inv, inv2 = scales
        factor = (-0.5625 * inv2 * inv) * tiles(col1, pairs, 0) + (
            0.0625 * inv2 * inv2
        ) * tiles(col2, pairs, 0)
        return dot3(tiles(row2, pairs, 1), factor)

    result = gather(
        row2, col2, c_send.at[1], c2_recv, r_send.at[1], r2_recv, send_norms, last
    )
    inv, inv2 = scales
    rows = lax.broadcasted_iota(jnp.int32, (B, B), 0)
    cols = lax.broadcasted_iota(jnp.int32, (B, B), 1)
    constant = jnp.where((rows == cols) & (ti == tj), 2.25, 0.0)
    result = constant + (-2.4375 * inv) * row1[tj] + (1.6875 * inv2) * row2[tj] + result
    r_own[...] = result
    r_out[...] = result
    r_swap = remote(r_own, r_far, swap_send.at[2], swap_recv.at[2], (ti, tj))

    @pl.when(swapped)
    def _():
        r_swap.start()
        s_swap.wait_send()
        s_swap.wait_recv()
        s_out[...] = s_far[...]

    for phase, (row, col) in enumerate(((row1, col1), (row2, col2))):
        bytes_of(row.at[pl.ds(0, 15)], r_send.at[phase])
        bytes_of(col.at[pl.ds(0, 15)], c_send.at[phase])
    bytes_of(norms.at[pl.ds(0, N - 1)], n_send)
    bytes_of(gj.at[pl.ds(0, quarter)], g_send)
    bytes_of(gi.at[pl.ds(0, 22 * PIECE - 8 * PIECE)], g_send)
    bytes_of(gj.at[pl.ds(0, 8 * PIECE)], g_send)

    @pl.when(swapped)
    def _():
        bytes_of(g_own, g_send)

    @pl.when(i != tj)
    def _():
        bytes_of(g_own, g_send)

    @pl.when(swapped)
    def _():
        r_swap.wait_send()
        r_swap.wait_recv()
        r_out[...] = r_far[...]


def store(s_ref, r_ref, s_hbm, r_hbm, sems):
    copies = [
        pltpu.make_async_copy(s_ref, s_hbm, sems.at[0]),
        pltpu.make_async_copy(r_ref, r_hbm, sems.at[1]),
    ]
    for copy in copies:
        copy.start()
    for copy in copies:
        copy.wait()


def local(gradient, stat_old):
    dma = pltpu.SemaphoreType.DMA
    n_col, n_row = len(COL_KEYS), len(ROW_KEYS)
    block = jax.ShapeDtypeStruct((B, B), jnp.float32)
    tile = pltpu.VMEM((B, B), jnp.float32)
    panel = pltpu.VMEM((N, B, B), jnp.float32)
    pieces = pltpu.VMEM((N * PIECE, B), jnp.float32)
    made = pl.pallas_call(
        kernel,
        out_shape=(block, block),
        in_specs=[pl.BlockSpec(memory_space=pltpu.HBM)] * 2,
        out_specs=[pl.BlockSpec(memory_space=pltpu.VMEM)] * 2,
        scratch_shapes=[
            pltpu.VMEM((PIECE, B), jnp.float32), tile, tile, tile, tile, tile,
            pieces, pieces, panel, panel, panel, panel, pltpu.VMEM((N, 1, B), jnp.float32),
            dma((3,)), dma(()), dma(()), dma(()), dma(()),
            dma((2,)), dma((2,)), dma((n_col,)), dma((n_row,)), dma((n_col,)), dma((n_row,)),
            dma(()), dma(()), dma((3,)), dma((3,)),
        ],
        compiler_params=pltpu.CompilerParams(
            collective_id=0, has_side_effects=True, vmem_limit_bytes=16 * 1024 * 1024
        ),
        name="shampoo",
    )(
        pltpu.with_memory_space_constraint(gradient.T, pltpu.HBM),
        pltpu.with_memory_space_constraint(stat_old, pltpu.HBM),
    )
    return pl.pallas_call(
        store,
        out_shape=(block, block),
        in_specs=[pl.BlockSpec(memory_space=pltpu.VMEM)] * 2,
        out_specs=[pl.BlockSpec(memory_space=pltpu.HBM)] * 2,
        scratch_shapes=[dma((2,))],
        compiler_params=pltpu.CompilerParams(vmem_limit_bytes=1024 * 1024),
        name="store",
    )(*made)


def solution(mesh):
    placed = (P("gx", "gy"), P("gx", "gy"))
    return jax.shard_map(local, mesh=mesh, in_specs=placed, out_specs=placed, check_vma=False)
```

```python
import functools

import jax
import jax.numpy as jnp
from jax import lax
from jax.experimental import pallas as pl
from jax.experimental.pallas import tpu as pltpu
from jax.sharding import PartitionSpec as P

MESH = pl.DeviceIdType.MESH
N = 16
B = 128
HALF = B // 2
PIECE = 32
STEPS = (1, 3, 2)

ROW_KEYS = [("x", s) for s in STEPS] + [("y", s) for s in STEPS] + ["rest"]
COL_KEYS = (
    [("z", 2, d, h) for d in (0, 1) for h in (0, 1)]
    + [("z", 1), ("z", 3, 0), ("z", 3, 1), ("z", 4), "near", "far"]
)
ROW_AT = {key: number for number, key in enumerate(ROW_KEYS)}
COL_AT = {key: number for number, key in enumerate(COL_KEYS)}


def split(x):
    high = x.astype(jnp.bfloat16)
    low = (x - high.astype(jnp.float32)).astype(jnp.bfloat16)
    return high, low


def dot3(a, b, dims=(((1,), (0,)), ((), ()))):
    a_high, a_low = split(a)
    b_high, b_low = split(b)
    dot = functools.partial(
        lax.dot_general, dimension_numbers=dims, preferred_element_type=jnp.float32
    )
    return dot(a_high, b_high) + (dot(a_high, b_low) + dot(a_low, b_high))


def kernel(
    g_hbm, o_hbm, s_out, r_out,
    g_own, o_own, o_far, s_far, r_own, r_far,
    gi, gj, row1, col1, row2, col2, norms,
    local_sem, g_send, gi_recv, gj_recv, gc_recv,
    c_send, r_send, c1_recv, r1_recv, c2_recv, r2_recv,
    n_send, n_recv, swap_send, swap_recv,
):
    i = lax.axis_index("gx")
    j = lax.axis_index("gy")
    z, xl = lax.div(i, 2), lax.rem(i, 2)
    y, xh, c = lax.div(j, 4), lax.rem(lax.div(j, 2), 2), lax.rem(j, 2)
    x = xh * 2 + xl
    ti = z * 2 + c
    tj = y * 4 + x
    swapped = c != xl

    def at(pz, px, py, pc):
        return (pz * 2 + lax.rem(px, 2), py * 4 + lax.div(px, 2) * 2 + pc)

    def step(value, by, size):
        return lax.rem(value + by, size)

    def remote(src, dst, send_sem, recv_sem, to):
        return pltpu.make_async_remote_copy(
            src_ref=src, dst_ref=dst, send_sem=send_sem, recv_sem=recv_sem,
            device_id=to, device_id_type=MESH,
        )

    def bytes_of(ref, sem):
        pltpu.make_async_copy(ref, ref, sem).wait()

    g_in = pltpu.make_async_copy(g_hbm, g_own, local_sem.at[0])
    o_in = pltpu.make_async_copy(o_hbm, o_own, local_sem.at[1])
    g_in.start()
    o_in.start()

    barrier = pltpu.get_barrier_semaphore()

    def greet(to):
        pl.semaphore_signal(barrier, inc=1, device_id=to, device_id_type=MESH)

    for r in range(1, 8):
        greet((tj, step(j, 2 * r, N)))

    @pl.when(i != tj)
    def _():
        greet((tj, j))

    for r in range(1, N):
        greet((ti, step(j, r, N)))

    @pl.when(swapped)
    def _():
        greet((ti, j))
        greet((ti, tj))

    for s in STEPS:
        greet(at(z, step(x, s, 4), y, c))
        greet(at(z, x, step(y, s, 4), c))
    for s in range(1, 8):
        greet(at(step(z, s, 8), x, y, c))
    for s in range(8):
        greet(at(step(z, s, 8), x, y, 1 - c))
    g_in.wait()
    same = 1 - (c - xl) * (c - xl)
    pl.semaphore_wait(barrier, 46 - 2 * same - (i == tj).astype(jnp.int32))

    order = lax.rem(j, 2) * 8 + lax.div(j, 2)
    mine = pl.ds(pl.multiple_of(order * PIECE, PIECE), PIECE)
    ky, kx = lax.div(i, 4), lax.rem(i, 4)
    gi_near = remote(g_own, gi.at[mine], g_send, gi_recv, (i, y * 4 + xh * 2 + xl))
    gj_near = remote(g_own, gj.at[mine], g_send, gj_recv, at(z, kx, ky, c))
    gi_here = pltpu.make_async_copy(g_own, gi.at[mine], local_sem.at[0])
    gj_here = pltpu.make_async_copy(g_own, gj.at[mine], local_sem.at[2])

    for r in (4, 3, 5, 2, 6, 1, 7):
        remote(g_own, gj.at[mine], g_send, gj_recv, at(step(z, r, 8), kx, ky, c)).start()

    @pl.when(i != tj)
    def _():
        gj_near.start()

    @pl.when(i == tj)
    def _():
        gj_here.start()

    for r in (10, 2, 8, 6, 14, 9, 11, 5, 7, 13, 15, 1, 3, 4, 12, 0):
        sx, sy = r % 4, r // 4
        if r:
            remote(
                g_own, gi.at[mine], g_send, gi_recv, at(z, step(x, sx, 4), step(y, sy, 4), xl)
            ).start()

    @pl.when(swapped)
    def _():
        gi_near.start()

    @pl.when(jnp.logical_not(swapped))
    def _():
        gi_here.start()

    o_in.wait()
    o_swap = remote(o_own, o_far, swap_send.at[0], swap_recv.at[0], (ti, tj))

    @pl.when(swapped)
    def _():
        o_swap.start()

    quarter = 8 * PIECE

    @pl.when(i != tj)
    def _():
        bytes_of(gj.at[pl.ds(0, quarter)], gj_recv)

    @pl.when(i == tj)
    def _():
        bytes_of(gj.at[pl.ds(0, quarter - PIECE)], gj_recv)
        gj_here.wait()

    mine_half = pl.ds(pl.multiple_of(c * quarter, quarter), quarter)
    other_half = pl.ds(pl.multiple_of((1 - c) * quarter, quarter), quarter)
    gj_share = remote(gj.at[mine_half], gj.at[mine_half], g_send, gc_recv, (i, j + 1 - 2 * c))
    gj_share.start()

    @pl.when(swapped)
    def _():
        bytes_of(gi, gi_recv)

    @pl.when(jnp.logical_not(swapped))
    def _():
        bytes_of(gi.at[pl.ds(0, 15 * PIECE)], gi_recv)
        gi_here.wait()

    rows_of = (((0,), (0,)), ((), ()))
    outer = dot3(gi[mine_half, :], gj[mine_half, :], rows_of)
    remote(
        gj.at[other_half], gj.at[other_half], g_send, gc_recv, (i, j + 1 - 2 * c)
    ).wait_recv()
    outer = outer + dot3(gi[other_half, :], gj[other_half, :], rows_of)

    @pl.when(swapped)
    def _():
        o_swap.wait_send()
        o_swap.wait_recv()
        o_own[...] = o_far[...]

    stat = 0.9 * o_own[...] + outer * (1.0 / (N * PIECE))

    def gather(row, col, c_send, c_recv, r_send, r_recv, between, product):
        def row_send(key, slot, h, to):
            part = row.at[slot, pl.ds(h * HALF, HALF)]
            remote(part, part, r_send, r_recv.at[ROW_AT[key]], to).start()

        def row_wait(key, tiles):
            bytes_of(tiles, r_recv.at[ROW_AT[key]])

        def col_part(slot, h):
            return col.at[slot] if h is None else col.at[slot, pl.ds(h * HALF, HALF)]

        def col_send(key, slot, h, to):
            part = col_part(slot, h)
            remote(part, part, c_send, c_recv.at[COL_AT[key]], to).start()

        def col_wait(key, tiles):
            bytes_of(tiles, c_recv.at[COL_AT[key]])

        def x_to(s):
            return at(z, step(x, s, 4), y, c)

        def y_to(s):
            return at(z, x, step(y, s, 4), c)

        def z_to(s):
            return at(step(z, s, 8), x, y, c)

        def from_xy(dx, dy):
            return step(y, 4 - dy, 4) * 4 + step(x, 4 - dx, 4)

        def from_z(dz, core):
            return step(z, 8 - dz, 8) * 2 + core

        other = (i, j + 1 - 2 * c)
        away = (2, 6)
        near = (1, 7)
        for h in (0, 1):
            for d in (0, 1):
                col_send(("z", 2, d, h), ti, h, z_to(away[d]))
            for s in STEPS:
                row_send(("x", s) if h == 0 else "rest", tj, h, x_to(s))
                row_send(("y", s) if h == 0 else "rest", tj, 1 - h, y_to(s))
        for d in (0, 1):
            col_send(("z", 1), ti, None, z_to(near[d]))
        col_send("near", ti, None, other)
        between()

        half = row.at[0, pl.ds(0, HALF)]
        def relay_xy(s):
            row_wait(("x", s), half)
            for t in (2, 1, 3):
                row_send("rest", from_xy(s, 0), 0, y_to(t))
            row_wait(("y", s), half)
            for t in (2, 1, 3):
                row_send("rest", from_xy(0, s), 1, x_to(t))

        def relay_z(h):
            for d in (0, 1):
                slot = from_z(away[d], c)
                col_wait(("z", 2, d, h), half)
                if h == d:
                    col_send(("z", 4), slot, h, z_to(away[d]))
                col_send(("z", 3, d), slot, h, z_to(near[d]))

        relay_xy(STEPS[0])
        relay_xy(STEPS[1])
        relay_z(0)
        relay_xy(STEPS[2])
        relay_z(1)
        for d in (0, 1):
            col_send("near", from_z(away[d], c), None, other)
        col_wait(("z", 1), col.at[pl.ds(0, 2)])
        for d in (0, 1):
            col_send("near", from_z(near[d], c), None, other)
        for d in (0, 1):
            col_wait(("z", 3, d), col.at[0])
            col_send("far", from_z((away[d] + near[d]) % 8, c), None, other)
        col_wait(("z", 4), col.at[0])
        col_send("far", from_z(4, c), None, other)
        row_wait("rest", row.at[pl.ds(0, 12)])
        col_wait("near", col.at[pl.ds(0, 5)])
        total = product([step(z, dz, 8) for dz in (0, 1, 7, 2, 6)])
        col_wait("far", col.at[pl.ds(0, 3)])
        return total + product([step(z, dz, 8) for dz in (3, 5, 4)])

    row1[tj] = stat
    col1[ti] = stat
    s_swap = remote(row1.at[tj], s_far, swap_send.at[1], swap_recv.at[1], (ti, tj))

    def tiles(ref, pairs, axis):
        return jnp.concatenate([ref[2 * k + h] for k in pairs for h in (0, 1)], axis=axis)

    def keep_stat():
        s_out[...] = stat

        @pl.when(swapped)
        def _():
            s_swap.start()

    def square(pairs):
        return dot3(tiles(row1, pairs, 1), tiles(col1, pairs, 0))

    power = gather(
        row1, col1, c_send.at[0], c1_recv, r_send.at[0], r1_recv, keep_stat, square
    )
    row2[tj] = power
    col2[ti] = power

    def send_norms():
        squares = jnp.zeros((B, B), jnp.float32)
        for k in range(N):
            squares = squares + row1[k] * row1[k]
        norms[ti] = jnp.sum(squares, axis=0, keepdims=True)
        for r in range(1, N):
            remote(
                norms.at[ti], norms.at[ti], n_send, n_recv,
                at(step(z, r // 2, 8), x, y, step(c, r % 2, 2)),
            ).start()

    scales = []

    def last(pairs):
        if not scales:
            bytes_of(norms.at[pl.ds(0, N - 1)], n_recv)
            total = jnp.sum(jnp.sum(norms[...], axis=0), axis=1, keepdims=True)
            inv = 1.0 / (2.0 * jnp.sqrt(total * (1.0 / (N * B))))
            scales.extend((inv, inv * inv))
        inv, inv2 = scales
        factor = (-0.5625 * inv2 * inv) * tiles(col1, pairs, 0) + (
            0.0625 * inv2 * inv2
        ) * tiles(col2, pairs, 0)
        return dot3(tiles(row2, pairs, 1), factor)

    result = gather(
        row2, col2, c_send.at[1], c2_recv, r_send.at[1], r2_recv, send_norms, last
    )
    inv, inv2 = scales
    rows = lax.broadcasted_iota(jnp.int32, (B, B), 0)
    cols = lax.broadcasted_iota(jnp.int32, (B, B), 1)
    constant = jnp.where((rows == cols) & (ti == tj), 2.25, 0.0)
    result = constant + (-2.4375 * inv) * row1[tj] + (1.6875 * inv2) * row2[tj] + result
    r_own[...] = result
    r_out[...] = result
    r_swap = remote(r_own, r_far, swap_send.at[2], swap_recv.at[2], (ti, tj))

    @pl.when(swapped)
    def _():
        r_swap.start()
        s_swap.wait_send()
        s_swap.wait_recv()
        s_out[...] = s_far[...]

    for phase, (row, col) in enumerate(((row1, col1), (row2, col2))):
        bytes_of(row.at[pl.ds(0, 15)], r_send.at[phase])
        bytes_of(col.at[pl.ds(0, 15)], c_send.at[phase])
    bytes_of(norms.at[pl.ds(0, N - 1)], n_send)
    bytes_of(gj.at[pl.ds(0, quarter)], g_send)
    bytes_of(gi.at[pl.ds(0, 22 * PIECE - 8 * PIECE)], g_send)
    bytes_of(gj.at[pl.ds(0, 8 * PIECE)], g_send)

    @pl.when(swapped)
    def _():
        bytes_of(g_own, g_send)

    @pl.when(i != tj)
    def _():
        bytes_of(g_own, g_send)

    @pl.when(swapped)
    def _():
        r_swap.wait_send()
        r_swap.wait_recv()
        r_out[...] = r_far[...]


def store(s_ref, r_ref, s_hbm, r_hbm, sems):
    copies = [
        pltpu.make_async_copy(s_ref, s_hbm, sems.at[0]),
        pltpu.make_async_copy(r_ref, r_hbm, sems.at[1]),
    ]
    for copy in copies:
        copy.start()
    for copy in copies:
        copy.wait()


def local(gradient, stat_old):
    dma = pltpu.SemaphoreType.DMA
    n_col, n_row = len(COL_KEYS), len(ROW_KEYS)
    block = jax.ShapeDtypeStruct((B, B), jnp.float32)
    tile = pltpu.VMEM((B, B), jnp.float32)
    panel = pltpu.VMEM((N, B, B), jnp.float32)
    pieces = pltpu.VMEM((N * PIECE, B), jnp.float32)
    made = pl.pallas_call(
        kernel,
        out_shape=(block, block),
        in_specs=[pl.BlockSpec(memory_space=pltpu.HBM)] * 2,
        out_specs=[pl.BlockSpec(memory_space=pltpu.VMEM)] * 2,
        scratch_shapes=[
            pltpu.VMEM((PIECE, B), jnp.float32), tile, tile, tile, tile, tile,
            pieces, pieces, panel, panel, panel, panel, pltpu.VMEM((N, 1, B), jnp.float32),
            dma((3,)), dma(()), dma(()), dma(()), dma(()),
            dma((2,)), dma((2,)), dma((n_col,)), dma((n_row,)), dma((n_col,)), dma((n_row,)),
            dma(()), dma(()), dma((3,)), dma((3,)),
        ],
        compiler_params=pltpu.CompilerParams(
            collective_id=0, has_side_effects=True, vmem_limit_bytes=16 * 1024 * 1024
        ),
        name="shampoo",
    )(
        pltpu.with_memory_space_constraint(gradient.T, pltpu.HBM),
        pltpu.with_memory_space_constraint(stat_old, pltpu.HBM),
    )
    return pl.pallas_call(
        store,
        out_shape=(block, block),
        in_specs=[pl.BlockSpec(memory_space=pltpu.VMEM)] * 2,
        out_specs=[pl.BlockSpec(memory_space=pltpu.HBM)] * 2,
        scratch_shapes=[dma((2,))],
        compiler_params=pltpu.CompilerParams(vmem_limit_bytes=1024 * 1024),
        name="store",
    )(*made)


def solution(mesh):
    placed = (P("gx", "gy"), P("gx", "gy"))
    return jax.shard_map(local, mesh=mesh, in_specs=placed, out_specs=placed, check_vma=False)
```

```python
import functools

import jax
import jax.numpy as jnp
from jax import lax
from jax.experimental import pallas as pl
from jax.experimental.pallas import tpu as pltpu
from jax.sharding import PartitionSpec as P

MESH = pl.DeviceIdType.MESH
N = 16
B = 128
HALF = B // 2
PIECE = 32
STEPS = (1, 3, 2)

ROW_KEYS = [("x", s) for s in STEPS] + [("y", s) for s in STEPS] + ["rest"]
COL_KEYS = (
    [("z", 2, d, h) for d in (0, 1) for h in (0, 1)]
    + [("z", 1), ("z", 3, 0), ("z", 3, 1), ("z", 4), "near", "far"]
)
ROW_AT = {key: number for number, key in enumerate(ROW_KEYS)}
COL_AT = {key: number for number, key in enumerate(COL_KEYS)}


def split(x):
    high = x.astype(jnp.bfloat16)
    low = (x - high.astype(jnp.float32)).astype(jnp.bfloat16)
    return high, low


def dot3(a, b, dims=(((1,), (0,)), ((), ()))):
    a_high, a_low = split(a)
    b_high, b_low = split(b)
    dot = functools.partial(
        lax.dot_general, dimension_numbers=dims, preferred_element_type=jnp.float32
    )
    return dot(a_high, b_high) + (dot(a_high, b_low) + dot(a_low, b_high))


def kernel(
    g_hbm, o_hbm, s_out, r_out,
    g_own, o_own, o_far, s_far, r_own, r_far,
    gi, gj, row1, col1, row2, col2, norms,
    local_sem, g_send, gi_recv, gj_recv, gc_recv,
    c_send, r_send, c1_recv, r1_recv, c2_recv, r2_recv,
    n_send, n_recv, swap_send, swap_recv,
):
    i = lax.axis_index("gx")
    j = lax.axis_index("gy")
    z, xl = lax.div(i, 2), lax.rem(i, 2)
    y, xh, c = lax.div(j, 4), lax.rem(lax.div(j, 2), 2), lax.rem(j, 2)
    x = xh * 2 + xl
    ti = z * 2 + c
    tj = y * 4 + x
    swapped = c != xl

    def at(pz, px, py, pc):
        return (pz * 2 + lax.rem(px, 2), py * 4 + lax.div(px, 2) * 2 + pc)

    def step(value, by, size):
        return lax.rem(value + by, size)

    def remote(src, dst, send_sem, recv_sem, to):
        return pltpu.make_async_remote_copy(
            src_ref=src, dst_ref=dst, send_sem=send_sem, recv_sem=recv_sem,
            device_id=to, device_id_type=MESH,
        )

    def bytes_of(ref, sem):
        pltpu.make_async_copy(ref, ref, sem).wait()

    g_in = pltpu.make_async_copy(g_hbm, g_own, local_sem.at[0])
    o_in = pltpu.make_async_copy(o_hbm, o_own, local_sem.at[1])
    g_in.start()
    o_in.start()

    barrier = pltpu.get_barrier_semaphore()

    def greet(to):
        pl.semaphore_signal(barrier, inc=1, device_id=to, device_id_type=MESH)

    for r in range(1, 8):
        greet((tj, step(j, 2 * r, N)))

    @pl.when(i != tj)
    def _():
        greet((tj, j))

    for r in range(1, N):
        greet((ti, step(j, r, N)))

    @pl.when(swapped)
    def _():
        greet((ti, j))
        greet((ti, tj))

    for s in STEPS:
        greet(at(z, step(x, s, 4), y, c))
        greet(at(z, x, step(y, s, 4), c))
    for s in range(1, 8):
        greet(at(step(z, s, 8), x, y, c))
    for s in range(8):
        greet(at(step(z, s, 8), x, y, 1 - c))
    g_in.wait()
    same = 1 - (c - xl) * (c - xl)
    pl.semaphore_wait(barrier, 46 - 2 * same - (i == tj).astype(jnp.int32))

    order = lax.rem(j, 2) * 8 + lax.div(j, 2)
    mine = pl.ds(pl.multiple_of(order * PIECE, PIECE), PIECE)
    ky, kx = lax.div(i, 4), lax.rem(i, 4)
    gi_near = remote(g_own, gi.at[mine], g_send, gi_recv, (i, y * 4 + xh * 2 + xl))
    gj_near = remote(g_own, gj.at[mine], g_send, gj_recv, at(z, kx, ky, c))
    gi_here = pltpu.make_async_copy(g_own, gi.at[mine], local_sem.at[0])
    gj_here = pltpu.make_async_copy(g_own, gj.at[mine], local_sem.at[2])

    for r in (4, 3, 5, 2, 6, 1, 7):
        remote(g_own, gj.at[mine], g_send, gj_recv, at(step(z, r, 8), kx, ky, c)).start()

    @pl.when(i != tj)
    def _():
        gj_near.start()

    @pl.when(i == tj)
    def _():
        gj_here.start()

    for r in (10, 2, 8, 6, 14, 9, 11, 5, 7, 13, 15, 1, 3, 4, 12, 0):
        sx, sy = r % 4, r // 4
        if r:
            remote(
                g_own, gi.at[mine], g_send, gi_recv, at(z, step(x, sx, 4), step(y, sy, 4), xl)
            ).start()

    @pl.when(swapped)
    def _():
        gi_near.start()

    @pl.when(jnp.logical_not(swapped))
    def _():
        gi_here.start()

    o_in.wait()
    o_swap = remote(o_own, o_far, swap_send.at[0], swap_recv.at[0], (ti, tj))

    @pl.when(swapped)
    def _():
        o_swap.start()

    quarter = 8 * PIECE

    @pl.when(i != tj)
    def _():
        bytes_of(gj.at[pl.ds(0, quarter)], gj_recv)

    @pl.when(i == tj)
    def _():
        bytes_of(gj.at[pl.ds(0, quarter - PIECE)], gj_recv)
        gj_here.wait()

    mine_half = pl.ds(pl.multiple_of(c * quarter, quarter), quarter)
    other_half = pl.ds(pl.multiple_of((1 - c) * quarter, quarter), quarter)
    gj_share = remote(gj.at[mine_half], gj.at[mine_half], g_send, gc_recv, (i, j + 1 - 2 * c))
    gj_share.start()

    @pl.when(swapped)
    def _():
        bytes_of(gi, gi_recv)

    @pl.when(jnp.logical_not(swapped))
    def _():
        bytes_of(gi.at[pl.ds(0, 15 * PIECE)], gi_recv)
        gi_here.wait()

    rows_of = (((0,), (0,)), ((), ()))
    outer = dot3(gi[mine_half, :], gj[mine_half, :], rows_of)
    remote(
        gj.at[other_half], gj.at[other_half], g_send, gc_recv, (i, j + 1 - 2 * c)
    ).wait_recv()
    outer = outer + dot3(gi[other_half, :], gj[other_half, :], rows_of)

    @pl.when(swapped)
    def _():
        o_swap.wait_send()
        o_swap.wait_recv()
        o_own[...] = o_far[...]

    stat = 0.9 * o_own[...] + outer * (1.0 / (N * PIECE))

    def gather(row, col, c_send, c_recv, r_send, r_recv, between, product):
        def row_send(key, slot, h, to):
            part = row.at[slot, pl.ds(h * HALF, HALF)]
            remote(part, part, r_send, r_recv.at[ROW_AT[key]], to).start()

        def row_wait(key, tiles):
            bytes_of(tiles, r_recv.at[ROW_AT[key]])

        def col_part(slot, h):
            return col.at[slot] if h is None else col.at[slot, pl.ds(h * HALF, HALF)]

        def col_send(key, slot, h, to):
            part = col_part(slot, h)
            remote(part, part, c_send, c_recv.at[COL_AT[key]], to).start()

        def col_wait(key, tiles):
            bytes_of(tiles, c_recv.at[COL_AT[key]])

        def x_to(s):
            return at(z, step(x, s, 4), y, c)

        def y_to(s):
            return at(z, x, step(y, s, 4), c)

        def z_to(s):
            return at(step(z, s, 8), x, y, c)

        def from_xy(dx, dy):
            return step(y, 4 - dy, 4) * 4 + step(x, 4 - dx, 4)

        def from_z(dz, core):
            return step(z, 8 - dz, 8) * 2 + core

        other = (i, j + 1 - 2 * c)
        away = (2, 6)
        near = (1, 7)
        for h in (0, 1):
            for d in (0, 1):
                col_send(("z", 2, d, h), ti, h, z_to(away[d]))
            for s in STEPS:
                row_send(("x", s) if h == 0 else "rest", tj, h, x_to(s))
                row_send(("y", s) if h == 0 else "rest", tj, 1 - h, y_to(s))
        for d in (0, 1):
            col_send(("z", 1), ti, None, z_to(near[d]))
        col_send("near", ti, None, other)
        between()

        half = row.at[0, pl.ds(0, HALF)]
        def relay_xy(s):
            row_wait(("x", s), half)
            for t in (2, 1, 3):
                row_send("rest", from_xy(s, 0), 0, y_to(t))
            row_wait(("y", s), half)
            for t in (2, 1, 3):
                row_send("rest", from_xy(0, s), 1, x_to(t))

        def relay_z(h):
            for d in (0, 1):
                slot = from_z(away[d], c)
                col_wait(("z", 2, d, h), half)
                if h == d:
                    col_send(("z", 4), slot, h, z_to(away[d]))
                col_send(("z", 3, d), slot, h, z_to(near[d]))

        relay_xy(STEPS[0])
        relay_xy(STEPS[1])
        relay_z(0)
        relay_xy(STEPS[2])
        relay_z(1)
        for d in (0, 1):
            col_send("near", from_z(away[d], c), None, other)
        col_wait(("z", 1), col.at[pl.ds(0, 2)])
        for d in (0, 1):
            col_send("near", from_z(near[d], c), None, other)
        for d in (0, 1):
            col_wait(("z", 3, d), col.at[0])
            col_send("far", from_z((away[d] + near[d]) % 8, c), None, other)
        col_wait(("z", 4), col.at[0])
        col_send("far", from_z(4, c), None, other)
        row_wait("rest", row.at[pl.ds(0, 12)])
        col_wait("near", col.at[pl.ds(0, 5)])
        total = product(
            [from_z(dz, core) for dz in (0, 1, 7, 2, 6) for core in (c, 1 - c)]
            + [from_z(dz, c) for dz in (3, 5, 4)]
        )
        col_wait("far", col.at[pl.ds(0, 3)])
        return total + product([from_z(dz, 1 - c) for dz in (3, 5, 4)])

    row1[tj] = stat
    col1[ti] = stat
    s_swap = remote(row1.at[tj], s_far, swap_send.at[1], swap_recv.at[1], (ti, tj))

    def tiles(ref, slots, axis):
        return jnp.concatenate([ref[slot] for slot in slots], axis=axis)

    def keep_stat():
        s_out[...] = stat

        @pl.when(swapped)
        def _():
            s_swap.start()

    def square(slots):
        return dot3(tiles(row1, slots, 1), tiles(col1, slots, 0))

    power = gather(
        row1, col1, c_send.at[0], c1_recv, r_send.at[0], r1_recv, keep_stat, square
    )
    row2[tj] = power
    col2[ti] = power

    def send_norms():
        squares = jnp.zeros((B, B), jnp.float32)
        for k in range(N):
            squares = squares + row1[k] * row1[k]
        norms[ti] = jnp.sum(squares, axis=0, keepdims=True)
        for r in range(1, N):
            remote(
                norms.at[ti], norms.at[ti], n_send, n_recv,
                at(step(z, r // 2, 8), x, y, step(c, r % 2, 2)),
            ).start()

    scales = []

    def last(slots):
        if not scales:
            bytes_of(norms.at[pl.ds(0, N - 1)], n_recv)
            total = jnp.sum(jnp.sum(norms[...], axis=0), axis=1, keepdims=True)
            inv = 1.0 / (2.0 * jnp.sqrt(total * (1.0 / (N * B))))
            scales.extend((inv, inv * inv))
        inv, inv2 = scales
        factor = (-0.5625 * inv2 * inv) * tiles(col1, slots, 0) + (
            0.0625 * inv2 * inv2
        ) * tiles(col2, slots, 0)
        return dot3(tiles(row2, slots, 1), factor)

    result = gather(
        row2, col2, c_send.at[1], c2_recv, r_send.at[1], r2_recv, send_norms, last
    )
    inv, inv2 = scales
    rows = lax.broadcasted_iota(jnp.int32, (B, B), 0)
    cols = lax.broadcasted_iota(jnp.int32, (B, B), 1)
    constant = jnp.where((rows == cols) & (ti == tj), 2.25, 0.0)
    result = constant + (-2.4375 * inv) * row1[tj] + (1.6875 * inv2) * row2[tj] + result
    r_own[...] = result
    r_out[...] = result
    r_swap = remote(r_own, r_far, swap_send.at[2], swap_recv.at[2], (ti, tj))

    @pl.when(swapped)
    def _():
        r_swap.start()
        s_swap.wait_send()
        s_swap.wait_recv()
        s_out[...] = s_far[...]

    for phase, (row, col) in enumerate(((row1, col1), (row2, col2))):
        bytes_of(row.at[pl.ds(0, 15)], r_send.at[phase])
        bytes_of(col.at[pl.ds(0, 15)], c_send.at[phase])
    bytes_of(norms.at[pl.ds(0, N - 1)], n_send)
    bytes_of(gj.at[pl.ds(0, quarter)], g_send)
    bytes_of(gi.at[pl.ds(0, 22 * PIECE - 8 * PIECE)], g_send)
    bytes_of(gj.at[pl.ds(0, 8 * PIECE)], g_send)

    @pl.when(swapped)
    def _():
        bytes_of(g_own, g_send)

    @pl.when(i != tj)
    def _():
        bytes_of(g_own, g_send)

    @pl.when(swapped)
    def _():
        r_swap.wait_send()
        r_swap.wait_recv()
        r_out[...] = r_far[...]


def store(s_ref, r_ref, s_hbm, r_hbm, sems):
    copies = [
        pltpu.make_async_copy(s_ref, s_hbm, sems.at[0]),
        pltpu.make_async_copy(r_ref, r_hbm, sems.at[1]),
    ]
    for copy in copies:
        copy.start()
    for copy in copies:
        copy.wait()


def local(gradient, stat_old):
    dma = pltpu.SemaphoreType.DMA
    n_col, n_row = len(COL_KEYS), len(ROW_KEYS)
    block = jax.ShapeDtypeStruct((B, B), jnp.float32)
    tile = pltpu.VMEM((B, B), jnp.float32)
    panel = pltpu.VMEM((N, B, B), jnp.float32)
    pieces = pltpu.VMEM((N * PIECE, B), jnp.float32)
    made = pl.pallas_call(
        kernel,
        out_shape=(block, block),
        in_specs=[pl.BlockSpec(memory_space=pltpu.HBM)] * 2,
        out_specs=[pl.BlockSpec(memory_space=pltpu.VMEM)] * 2,
        scratch_shapes=[
            pltpu.VMEM((PIECE, B), jnp.float32), tile, tile, tile, tile, tile,
            pieces, pieces, panel, panel, panel, panel, pltpu.VMEM((N, 1, B), jnp.float32),
            dma((3,)), dma(()), dma(()), dma(()), dma(()),
            dma((2,)), dma((2,)), dma((n_col,)), dma((n_row,)), dma((n_col,)), dma((n_row,)),
            dma(()), dma(()), dma((3,)), dma((3,)),
        ],
        compiler_params=pltpu.CompilerParams(
            collective_id=0, has_side_effects=True, vmem_limit_bytes=16 * 1024 * 1024
        ),
        name="shampoo",
    )(
        pltpu.with_memory_space_constraint(gradient.T, pltpu.HBM),
        pltpu.with_memory_space_constraint(stat_old, pltpu.HBM),
    )
    return pl.pallas_call(
        store,
        out_shape=(block, block),
        in_specs=[pl.BlockSpec(memory_space=pltpu.VMEM)] * 2,
        out_specs=[pl.BlockSpec(memory_space=pltpu.HBM)] * 2,
        scratch_shapes=[dma((2,))],
        compiler_params=pltpu.CompilerParams(vmem_limit_bytes=1024 * 1024),
        name="store",
    )(*made)


def solution(mesh):
    placed = (P("gx", "gy"), P("gx", "gy"))
    return jax.shard_map(local, mesh=mesh, in_specs=placed, out_specs=placed, check_vma=False)
```

```python
import functools

import jax
import jax.numpy as jnp
from jax import lax
from jax.experimental import pallas as pl
from jax.experimental.pallas import tpu as pltpu
from jax.sharding import PartitionSpec as P

MESH = pl.DeviceIdType.MESH
N = 16
B = 128
HALF = B // 2
PIECE = 32
STEPS = (1, 3, 2)

ROW_KEYS = [("x", s) for s in STEPS] + [("y", s) for s in STEPS] + ["rest"]
COL_KEYS = (
    [("z", 2, d, h) for d in (0, 1) for h in (0, 1)]
    + [("z", 1), ("z", 3, 0), ("z", 3, 1), ("z", 4), "near", "far"]
)
ROW_AT = {key: number for number, key in enumerate(ROW_KEYS)}
COL_AT = {key: number for number, key in enumerate(COL_KEYS)}


def split(x):
    high = x.astype(jnp.bfloat16)
    low = (x - high.astype(jnp.float32)).astype(jnp.bfloat16)
    return high, low


def dot3(a, b, dims=(((1,), (0,)), ((), ()))):
    a_high, a_low = split(a)
    b_high, b_low = split(b)
    dot = functools.partial(
        lax.dot_general, dimension_numbers=dims, preferred_element_type=jnp.float32
    )
    return dot(a_high, b_high) + (dot(a_high, b_low) + dot(a_low, b_high))


def kernel(
    g_hbm, o_hbm, s_out, r_out,
    g_own, o_own, o_far, s_far, r_own, r_far,
    gi, gj, row1, col1, row2, col2, norms,
    local_sem, g_send, gi_recv, gj_recv, gc_recv,
    c_send, r_send, c1_recv, r1_recv, c2_recv, r2_recv,
    n_send, n_recv, swap_send, swap_recv,
):
    i = lax.axis_index("gx")
    j = lax.axis_index("gy")
    z, xl = lax.div(i, 2), lax.rem(i, 2)
    y, xh, c = lax.div(j, 4), lax.rem(lax.div(j, 2), 2), lax.rem(j, 2)
    x = xh * 2 + xl
    ti = z * 2 + c
    tj = y * 4 + x
    swapped = c != xl

    def at(pz, px, py, pc):
        return (pz * 2 + lax.rem(px, 2), py * 4 + lax.div(px, 2) * 2 + pc)

    def step(value, by, size):
        return lax.rem(value + by, size)

    def remote(src, dst, send_sem, recv_sem, to):
        return pltpu.make_async_remote_copy(
            src_ref=src, dst_ref=dst, send_sem=send_sem, recv_sem=recv_sem,
            device_id=to, device_id_type=MESH,
        )

    def bytes_of(ref, sem):
        pltpu.make_async_copy(ref, ref, sem).wait()

    g_in = pltpu.make_async_copy(g_hbm, g_own, local_sem.at[0])
    o_in = pltpu.make_async_copy(o_hbm, o_own, local_sem.at[1])
    g_in.start()
    o_in.start()

    barrier = pltpu.get_barrier_semaphore()

    def greet(to):
        pl.semaphore_signal(barrier, inc=1, device_id=to, device_id_type=MESH)

    for r in range(1, 8):
        greet((tj, step(j, 2 * r, N)))

    @pl.when(i != tj)
    def _():
        greet((tj, j))

    for r in range(1, N):
        greet((ti, step(j, r, N)))

    @pl.when(swapped)
    def _():
        greet((ti, j))
        greet((ti, tj))

    for s in STEPS:
        greet(at(z, step(x, s, 4), y, c))
        greet(at(z, x, step(y, s, 4), c))
    for s in range(1, 8):
        greet(at(step(z, s, 8), x, y, c))
    for s in range(8):
        greet(at(step(z, s, 8), x, y, 1 - c))
    g_in.wait()
    same = 1 - (c - xl) * (c - xl)
    pl.semaphore_wait(barrier, 46 - 2 * same - (i == tj).astype(jnp.int32))

    order = lax.rem(j, 2) * 8 + lax.div(j, 2)
    mine = pl.ds(pl.multiple_of(order * PIECE, PIECE), PIECE)
    ky, kx = lax.div(i, 4), lax.rem(i, 4)
    gi_near = remote(g_own, gi.at[mine], g_send, gi_recv, (i, y * 4 + xh * 2 + xl))
    gj_near = remote(g_own, gj.at[mine], g_send, gj_recv, at(z, kx, ky, c))
    gi_here = pltpu.make_async_copy(g_own, gi.at[mine], local_sem.at[0])
    gj_here = pltpu.make_async_copy(g_own, gj.at[mine], local_sem.at[2])

    for r in (4, 3, 5, 2, 6, 1, 7):
        remote(g_own, gj.at[mine], g_send, gj_recv, at(step(z, r, 8), kx, ky, c)).start()

    @pl.when(i != tj)
    def _():
        gj_near.start()

    @pl.when(i == tj)
    def _():
        gj_here.start()

    for r in (10, 2, 8, 6, 14, 9, 11, 5, 7, 13, 15, 1, 3, 4, 12, 0):
        sx, sy = r % 4, r // 4
        if r:
            remote(
                g_own, gi.at[mine], g_send, gi_recv, at(z, step(x, sx, 4), step(y, sy, 4), xl)
            ).start()

    @pl.when(swapped)
    def _():
        gi_near.start()

    @pl.when(jnp.logical_not(swapped))
    def _():
        gi_here.start()

    o_in.wait()
    o_swap = remote(o_own, o_far, swap_send.at[0], swap_recv.at[0], (ti, tj))

    @pl.when(swapped)
    def _():
        o_swap.start()

    quarter = 8 * PIECE

    @pl.when(i != tj)
    def _():
        bytes_of(gj.at[pl.ds(0, quarter)], gj_recv)

    @pl.when(i == tj)
    def _():
        bytes_of(gj.at[pl.ds(0, quarter - PIECE)], gj_recv)
        gj_here.wait()

    mine_half = pl.ds(pl.multiple_of(c * quarter, quarter), quarter)
    other_half = pl.ds(pl.multiple_of((1 - c) * quarter, quarter), quarter)
    gj_share = remote(gj.at[mine_half], gj.at[mine_half], g_send, gc_recv, (i, j + 1 - 2 * c))
    gj_share.start()

    @pl.when(swapped)
    def _():
        bytes_of(gi, gi_recv)

    @pl.when(jnp.logical_not(swapped))
    def _():
        bytes_of(gi.at[pl.ds(0, 15 * PIECE)], gi_recv)
        gi_here.wait()

    rows_of = (((0,), (0,)), ((), ()))
    outer = dot3(gi[mine_half, :], gj[mine_half, :], rows_of)
    remote(
        gj.at[other_half], gj.at[other_half], g_send, gc_recv, (i, j + 1 - 2 * c)
    ).wait_recv()
    outer = outer + dot3(gi[other_half, :], gj[other_half, :], rows_of)

    @pl.when(swapped)
    def _():
        o_swap.wait_send()
        o_swap.wait_recv()
        o_own[...] = o_far[...]

    stat = 0.9 * o_own[...] + outer * (1.0 / (N * PIECE))

    def gather(row, col, c_send, c_recv, r_send, r_recv, between, prepare, product):
        def row_send(key, slot, h, to):
            part = row.at[slot, pl.ds(h * HALF, HALF)]
            remote(part, part, r_send, r_recv.at[ROW_AT[key]], to).start()

        def row_wait(key, tiles):
            bytes_of(tiles, r_recv.at[ROW_AT[key]])

        def col_part(slot, h):
            return col.at[slot] if h is None else col.at[slot, pl.ds(h * HALF, HALF)]

        def col_send(key, slot, h, to):
            part = col_part(slot, h)
            remote(part, part, c_send, c_recv.at[COL_AT[key]], to).start()

        def col_wait(key, tiles):
            bytes_of(tiles, c_recv.at[COL_AT[key]])

        def x_to(s):
            return at(z, step(x, s, 4), y, c)

        def y_to(s):
            return at(z, x, step(y, s, 4), c)

        def z_to(s):
            return at(step(z, s, 8), x, y, c)

        def from_xy(dx, dy):
            return step(y, 4 - dy, 4) * 4 + step(x, 4 - dx, 4)

        def from_z(dz, core):
            return step(z, 8 - dz, 8) * 2 + core

        other = (i, j + 1 - 2 * c)
        away = (2, 6)
        near = (1, 7)
        for h in (0, 1):
            for d in (0, 1):
                col_send(("z", 2, d, h), ti, h, z_to(away[d]))
            for s in STEPS:
                row_send(("x", s) if h == 0 else "rest", tj, h, x_to(s))
                row_send(("y", s) if h == 0 else "rest", tj, 1 - h, y_to(s))
        for d in (0, 1):
            col_send(("z", 1), ti, None, z_to(near[d]))
        col_send("near", ti, None, other)
        between()

        half = row.at[0, pl.ds(0, HALF)]
        def relay_xy(s):
            row_wait(("x", s), half)
            for t in (2, 1, 3):
                row_send("rest", from_xy(s, 0), 0, y_to(t))
            row_wait(("y", s), half)
            for t in (2, 1, 3):
                row_send("rest", from_xy(0, s), 1, x_to(t))

        def relay_z(h):
            for d in (0, 1):
                slot = from_z(away[d], c)
                col_wait(("z", 2, d, h), half)
                if h == d:
                    col_send(("z", 4), slot, h, z_to(away[d]))
                col_send(("z", 3, d), slot, h, z_to(near[d]))

        relay_xy(STEPS[0])
        relay_xy(STEPS[1])
        relay_z(0)
        relay_xy(STEPS[2])
        relay_z(1)
        for d in (0, 1):
            col_send("near", from_z(away[d], c), None, other)
        col_wait(("z", 1), col.at[pl.ds(0, 2)])
        for d in (0, 1):
            col_send("near", from_z(near[d], c), None, other)
        for d in (0, 1):
            col_wait(("z", 3, d), col.at[0])
            col_send("far", from_z((away[d] + near[d]) % 8, c), None, other)
        col_wait(("z", 4), col.at[0])
        col_send("far", from_z(4, c), None, other)
        prepare()
        row_wait("rest", row.at[pl.ds(0, 12)])
        col_wait("near", col.at[pl.ds(0, 5)])
        total = product(
            [from_z(dz, core) for dz in (0, 1, 7, 2, 6) for core in (c, 1 - c)]
            + [from_z(dz, c) for dz in (3, 5, 4)]
        )
        col_wait("far", col.at[pl.ds(0, 3)])
        return total + product([from_z(dz, 1 - c) for dz in (3, 5, 4)])

    row1[tj] = stat
    col1[ti] = stat
    s_swap = remote(row1.at[tj], s_far, swap_send.at[1], swap_recv.at[1], (ti, tj))

    def tiles(ref, slots, axis):
        return jnp.concatenate([ref[slot] for slot in slots], axis=axis)

    def keep_stat():
        s_out[...] = stat

        @pl.when(swapped)
        def _():
            s_swap.start()

    def square(slots):
        return dot3(tiles(row1, slots, 1), tiles(col1, slots, 0))

    power = gather(
        row1, col1, c_send.at[0], c1_recv, r_send.at[0], r1_recv, keep_stat, lambda: None, square
    )
    row2[tj] = power
    col2[ti] = power

    def send_norms():
        squares = jnp.zeros((B, B), jnp.float32)
        for k in range(N):
            squares = squares + row1[k] * row1[k]
        norms[ti] = jnp.sum(squares, axis=0, keepdims=True)
        for r in range(1, N):
            remote(
                norms.at[ti], norms.at[ti], n_send, n_recv,
                at(step(z, r // 2, 8), x, y, step(c, r % 2, 2)),
            ).start()

    scales = []

    def scale():
        bytes_of(norms.at[pl.ds(0, N - 1)], n_recv)
        total = jnp.sum(jnp.sum(norms[...], axis=0), axis=1, keepdims=True)
        inv = 1.0 / (2.0 * jnp.sqrt(total * (1.0 / (N * B))))
        scales.extend((inv, inv * inv))

    def last(slots):
        inv, inv2 = scales
        factor = (-0.5625 * inv2 * inv) * tiles(col1, slots, 0) + (
            0.0625 * inv2 * inv2
        ) * tiles(col2, slots, 0)
        return dot3(tiles(row2, slots, 1), factor)

    result = gather(
        row2, col2, c_send.at[1], c2_recv, r_send.at[1], r2_recv, send_norms, scale, last
    )
    inv, inv2 = scales
    rows = lax.broadcasted_iota(jnp.int32, (B, B), 0)
    cols = lax.broadcasted_iota(jnp.int32, (B, B), 1)
    constant = jnp.where((rows == cols) & (ti == tj), 2.25, 0.0)
    result = constant + (-2.4375 * inv) * row1[tj] + (1.6875 * inv2) * row2[tj] + result
    r_own[...] = result
    r_out[...] = result
    r_swap = remote(r_own, r_far, swap_send.at[2], swap_recv.at[2], (ti, tj))

    @pl.when(swapped)
    def _():
        r_swap.start()
        s_swap.wait_send()
        s_swap.wait_recv()
        s_out[...] = s_far[...]

    for phase, (row, col) in enumerate(((row1, col1), (row2, col2))):
        bytes_of(row.at[pl.ds(0, 15)], r_send.at[phase])
        bytes_of(col.at[pl.ds(0, 15)], c_send.at[phase])
    bytes_of(norms.at[pl.ds(0, N - 1)], n_send)
    bytes_of(gj.at[pl.ds(0, quarter)], g_send)
    bytes_of(gi.at[pl.ds(0, 22 * PIECE - 8 * PIECE)], g_send)
    bytes_of(gj.at[pl.ds(0, 8 * PIECE)], g_send)

    @pl.when(swapped)
    def _():
        bytes_of(g_own, g_send)

    @pl.when(i != tj)
    def _():
        bytes_of(g_own, g_send)

    @pl.when(swapped)
    def _():
        r_swap.wait_send()
        r_swap.wait_recv()
        r_out[...] = r_far[...]


def store(s_ref, r_ref, s_hbm, r_hbm, sems):
    copies = [
        pltpu.make_async_copy(s_ref, s_hbm, sems.at[0]),
        pltpu.make_async_copy(r_ref, r_hbm, sems.at[1]),
    ]
    for copy in copies:
        copy.start()
    for copy in copies:
        copy.wait()


def local(gradient, stat_old):
    dma = pltpu.SemaphoreType.DMA
    n_col, n_row = len(COL_KEYS), len(ROW_KEYS)
    block = jax.ShapeDtypeStruct((B, B), jnp.float32)
    tile = pltpu.VMEM((B, B), jnp.float32)
    panel = pltpu.VMEM((N, B, B), jnp.float32)
    pieces = pltpu.VMEM((N * PIECE, B), jnp.float32)
    made = pl.pallas_call(
        kernel,
        out_shape=(block, block),
        in_specs=[pl.BlockSpec(memory_space=pltpu.HBM)] * 2,
        out_specs=[pl.BlockSpec(memory_space=pltpu.VMEM)] * 2,
        scratch_shapes=[
            pltpu.VMEM((PIECE, B), jnp.float32), tile, tile, tile, tile, tile,
            pieces, pieces, panel, panel, panel, panel, pltpu.VMEM((N, 1, B), jnp.float32),
            dma((3,)), dma(()), dma(()), dma(()), dma(()),
            dma((2,)), dma((2,)), dma((n_col,)), dma((n_row,)), dma((n_col,)), dma((n_row,)),
            dma(()), dma(()), dma((3,)), dma((3,)),
        ],
        compiler_params=pltpu.CompilerParams(
            collective_id=0, has_side_effects=True, vmem_limit_bytes=16 * 1024 * 1024
        ),
        name="shampoo",
    )(
        pltpu.with_memory_space_constraint(gradient.T, pltpu.HBM),
        pltpu.with_memory_space_constraint(stat_old, pltpu.HBM),
    )
    return pl.pallas_call(
        store,
        out_shape=(block, block),
        in_specs=[pl.BlockSpec(memory_space=pltpu.VMEM)] * 2,
        out_specs=[pl.BlockSpec(memory_space=pltpu.HBM)] * 2,
        scratch_shapes=[dma((2,))],
        compiler_params=pltpu.CompilerParams(vmem_limit_bytes=1024 * 1024),
        name="store",
    )(*made)


def solution(mesh):
    placed = (P("gx", "gy"), P("gx", "gy"))
    return jax.shard_map(local, mesh=mesh, in_specs=placed, out_specs=placed, check_vma=False)
```

```python
import functools

import jax
import jax.numpy as jnp
from jax import lax
from jax.experimental import pallas as pl
from jax.experimental.pallas import tpu as pltpu
from jax.sharding import PartitionSpec as P

MESH = pl.DeviceIdType.MESH
N = 16
B = 128
HALF = B // 2
PIECE = 32
STEPS = (1, 3, 2)

ROW_KEYS = [("x", s) for s in STEPS] + [("y", s) for s in STEPS] + ["rest"]
COL_KEYS = (
    [("z", 2, d, h) for d in (0, 1) for h in (0, 1)]
    + [("z", 1), ("z", 3, 0), ("z", 3, 1), ("z", 4), "near", "far"]
)
ROW_AT = {key: number for number, key in enumerate(ROW_KEYS)}
COL_AT = {key: number for number, key in enumerate(COL_KEYS)}


def split(x):
    high = x.astype(jnp.bfloat16)
    low = (x - high.astype(jnp.float32)).astype(jnp.bfloat16)
    return high, low


def dot3(a, b, dims=(((1,), (0,)), ((), ()))):
    a_high, a_low = split(a)
    b_high, b_low = split(b)
    dot = functools.partial(
        lax.dot_general, dimension_numbers=dims, preferred_element_type=jnp.float32
    )
    return dot(a_high, b_high) + (dot(a_high, b_low) + dot(a_low, b_high))


def kernel(
    g_hbm, o_hbm, s_out, r_out,
    g_own, o_own, o_far, s_far, r_own, r_far,
    gi, gj, row1, col1, row2, col2, norms,
    local_sem, g_send, gi_recv, gj_recv, gc_recv,
    c_send, r_send, c1_recv, r1_recv, c2_recv, r2_recv,
    n_send, n_recv, swap_send, swap_recv,
):
    i = lax.axis_index("gx")
    j = lax.axis_index("gy")
    z, xl = lax.div(i, 2), lax.rem(i, 2)
    y, xh, c = lax.div(j, 4), lax.rem(lax.div(j, 2), 2), lax.rem(j, 2)
    x = xh * 2 + xl
    ti = z * 2 + c
    tj = y * 4 + x
    swapped = c != xl

    def at(pz, px, py, pc):
        return (pz * 2 + lax.rem(px, 2), py * 4 + lax.div(px, 2) * 2 + pc)

    def step(value, by, size):
        return lax.rem(value + by, size)

    def remote(src, dst, send_sem, recv_sem, to):
        return pltpu.make_async_remote_copy(
            src_ref=src, dst_ref=dst, send_sem=send_sem, recv_sem=recv_sem,
            device_id=to, device_id_type=MESH,
        )

    def bytes_of(ref, sem):
        pltpu.make_async_copy(ref, ref, sem).wait()

    g_in = pltpu.make_async_copy(g_hbm, g_own, local_sem.at[0])
    o_in = pltpu.make_async_copy(o_hbm, o_own, local_sem.at[1])
    g_in.start()
    o_in.start()

    barrier = pltpu.get_barrier_semaphore()

    def greet(to):
        pl.semaphore_signal(barrier, inc=1, device_id=to, device_id_type=MESH)

    for r in range(1, 8):
        greet((tj, step(j, 2 * r, N)))

    @pl.when(i != tj)
    def _():
        greet((tj, j))

    for r in range(1, N):
        greet((ti, step(j, r, N)))

    @pl.when(swapped)
    def _():
        greet((ti, j))

    for s in STEPS:
        greet(at(z, step(x, s, 4), y, c))
        greet(at(z, x, step(y, s, 4), c))
    for s in range(1, 8):
        greet(at(step(z, s, 8), x, y, c))
    for s in range(8):
        greet(at(step(z, s, 8), x, y, 1 - c))
    g_in.wait()
    same = 1 - (c - xl) * (c - xl)
    pl.semaphore_wait(barrier, 45 - same - (i == tj).astype(jnp.int32))

    order = lax.rem(j, 2) * 8 + lax.div(j, 2)
    mine = pl.ds(pl.multiple_of(order * PIECE, PIECE), PIECE)
    ky, kx = lax.div(i, 4), lax.rem(i, 4)
    gi_near = remote(g_own, gi.at[mine], g_send, gi_recv, (i, y * 4 + xh * 2 + xl))
    gj_near = remote(g_own, gj.at[mine], g_send, gj_recv, at(z, kx, ky, c))
    gi_here = pltpu.make_async_copy(g_own, gi.at[mine], local_sem.at[0])
    gj_here = pltpu.make_async_copy(g_own, gj.at[mine], local_sem.at[2])

    for r in (4, 3, 5, 2, 6, 1, 7):
        remote(g_own, gj.at[mine], g_send, gj_recv, at(step(z, r, 8), kx, ky, c)).start()

    @pl.when(i != tj)
    def _():
        gj_near.start()

    @pl.when(i == tj)
    def _():
        gj_here.start()

    for r in (10, 2, 8, 6, 14, 9, 11, 5, 7, 13, 15, 1, 3, 4, 12, 0):
        sx, sy = r % 4, r // 4
        if r:
            remote(
                g_own, gi.at[mine], g_send, gi_recv, at(z, step(x, sx, 4), step(y, sy, 4), xl)
            ).start()

    @pl.when(swapped)
    def _():
        gi_near.start()

    @pl.when(jnp.logical_not(swapped))
    def _():
        gi_here.start()

    o_in.wait()
    o_swap = remote(o_own, o_far, swap_send.at[0], swap_recv.at[0], (ti, tj))

    @pl.when(swapped)
    def _():
        o_swap.start()

    quarter = 8 * PIECE

    @pl.when(i != tj)
    def _():
        bytes_of(gj.at[pl.ds(0, quarter)], gj_recv)

    @pl.when(i == tj)
    def _():
        bytes_of(gj.at[pl.ds(0, quarter - PIECE)], gj_recv)
        gj_here.wait()

    mine_half = pl.ds(pl.multiple_of(c * quarter, quarter), quarter)
    other_half = pl.ds(pl.multiple_of((1 - c) * quarter, quarter), quarter)
    gj_share = remote(gj.at[mine_half], gj.at[mine_half], g_send, gc_recv, (i, j + 1 - 2 * c))
    gj_share.start()

    @pl.when(swapped)
    def _():
        bytes_of(gi, gi_recv)

    @pl.when(jnp.logical_not(swapped))
    def _():
        bytes_of(gi.at[pl.ds(0, 15 * PIECE)], gi_recv)
        gi_here.wait()

    rows_of = (((0,), (0,)), ((), ()))
    outer = dot3(gi[mine_half, :], gj[mine_half, :], rows_of)
    remote(
        gj.at[other_half], gj.at[other_half], g_send, gc_recv, (i, j + 1 - 2 * c)
    ).wait_recv()
    outer = outer + dot3(gi[other_half, :], gj[other_half, :], rows_of)

    @pl.when(swapped)
    def _():
        o_swap.wait_send()
        o_swap.wait_recv()
        o_own[...] = o_far[...]

    stat = 0.9 * o_own[...] + outer * (1.0 / (N * PIECE))

    def gather(row, col, c_send, c_recv, r_send, r_recv, between, prepare, product):
        def row_send(key, slot, h, to):
            part = row.at[slot, pl.ds(h * HALF, HALF)]
            remote(part, part, r_send, r_recv.at[ROW_AT[key]], to).start()

        def row_wait(key, tiles):
            bytes_of(tiles, r_recv.at[ROW_AT[key]])

        def col_part(slot, h):
            return col.at[slot] if h is None else col.at[slot, pl.ds(h * HALF, HALF)]

        def col_send(key, slot, h, to):
            part = col_part(slot, h)
            remote(part, part, c_send, c_recv.at[COL_AT[key]], to).start()

        def col_wait(key, tiles):
            bytes_of(tiles, c_recv.at[COL_AT[key]])

        def x_to(s):
            return at(z, step(x, s, 4), y, c)

        def y_to(s):
            return at(z, x, step(y, s, 4), c)

        def z_to(s):
            return at(step(z, s, 8), x, y, c)

        def from_xy(dx, dy):
            return step(y, 4 - dy, 4) * 4 + step(x, 4 - dx, 4)

        def from_z(dz, core):
            return step(z, 8 - dz, 8) * 2 + core

        other = (i, j + 1 - 2 * c)
        away = (2, 6)
        near = (1, 7)
        for h in (0, 1):
            for d in (0, 1):
                col_send(("z", 2, d, h), ti, h, z_to(away[d]))
            for s in STEPS:
                row_send(("x", s) if h == 0 else "rest", tj, h, x_to(s))
                row_send(("y", s) if h == 0 else "rest", tj, 1 - h, y_to(s))
        for d in (0, 1):
            col_send(("z", 1), ti, None, z_to(near[d]))
        col_send("near", ti, None, other)
        between()

        half = row.at[0, pl.ds(0, HALF)]
        def relay_xy(s):
            row_wait(("x", s), half)
            for t in (2, 1, 3):
                row_send("rest", from_xy(s, 0), 0, y_to(t))
            row_wait(("y", s), half)
            for t in (2, 1, 3):
                row_send("rest", from_xy(0, s), 1, x_to(t))

        def relay_z(h):
            for d in (0, 1):
                slot = from_z(away[d], c)
                col_wait(("z", 2, d, h), half)
                if h == d:
                    col_send(("z", 4), slot, h, z_to(away[d]))
                col_send(("z", 3, d), slot, h, z_to(near[d]))

        relay_xy(STEPS[0])
        relay_xy(STEPS[1])
        relay_z(0)
        relay_xy(STEPS[2])
        relay_z(1)
        for d in (0, 1):
            col_send("near", from_z(away[d], c), None, other)
        col_wait(("z", 1), col.at[pl.ds(0, 2)])
        for d in (0, 1):
            col_send("near", from_z(near[d], c), None, other)
        for d in (0, 1):
            col_wait(("z", 3, d), col.at[0])
            col_send("far", from_z((away[d] + near[d]) % 8, c), None, other)
        col_wait(("z", 4), col.at[0])
        col_send("far", from_z(4, c), None, other)
        prepare()
        row_wait("rest", row.at[pl.ds(0, 12)])
        col_wait("near", col.at[pl.ds(0, 5)])
        total = product(
            [from_z(dz, core) for dz in (0, 1, 7, 2, 6) for core in (c, 1 - c)]
            + [from_z(dz, c) for dz in (3, 5, 4)]
        )
        col_wait("far", col.at[pl.ds(0, 3)])
        return total + product([from_z(dz, 1 - c) for dz in (3, 5, 4)])

    row1[tj] = stat
    col1[ti] = stat
    s_swap = remote(row1.at[tj], s_far, swap_send.at[1], swap_recv.at[1], (ti, tj))

    def tiles(ref, slots, axis):
        return jnp.concatenate([ref[slot] for slot in slots], axis=axis)

    def keep_stat():
        s_out[...] = stat

        @pl.when(swapped)
        def _():
            s_swap.start()

    def square(slots):
        return dot3(tiles(row1, slots, 1), tiles(col1, slots, 0))

    power = gather(
        row1, col1, c_send.at[0], c1_recv, r_send.at[0], r1_recv, keep_stat, lambda: None, square
    )
    row2[tj] = power
    col2[ti] = power

    def send_norms():
        squares = jnp.zeros((B, B), jnp.float32)
        for k in range(N):
            squares = squares + row1[k] * row1[k]
        norms[ti] = jnp.sum(squares, axis=0, keepdims=True)
        for r in range(1, N):
            remote(
                norms.at[ti], norms.at[ti], n_send, n_recv,
                at(step(z, r // 2, 8), x, y, step(c, r % 2, 2)),
            ).start()

    scales = []

    def scale():
        bytes_of(norms.at[pl.ds(0, N - 1)], n_recv)
        total = jnp.sum(jnp.sum(norms[...], axis=0), axis=1, keepdims=True)
        inv = 1.0 / (2.0 * jnp.sqrt(total * (1.0 / (N * B))))
        scales.extend((inv, inv * inv))

    def last(slots):
        inv, inv2 = scales
        factor = (-0.5625 * inv2 * inv) * tiles(col1, slots, 0) + (
            0.0625 * inv2 * inv2
        ) * tiles(col2, slots, 0)
        return dot3(tiles(row2, slots, 1), factor)

    result = gather(
        row2, col2, c_send.at[1], c2_recv, r_send.at[1], r2_recv, send_norms, scale, last
    )
    inv, inv2 = scales
    rows = lax.broadcasted_iota(jnp.int32, (B, B), 0)
    cols = lax.broadcasted_iota(jnp.int32, (B, B), 1)
    constant = jnp.where((rows == cols) & (ti == tj), 2.25, 0.0)
    result = constant + (-2.4375 * inv) * row1[tj] + (1.6875 * inv2) * row2[tj] + result
    r_own[...] = result
    r_out[...] = result
    r_swap = remote(r_own, r_far, swap_send.at[2], swap_recv.at[2], (ti, tj))

    @pl.when(swapped)
    def _():
        r_swap.start()
        s_swap.wait_send()
        s_swap.wait_recv()
        s_out[...] = s_far[...]

    for phase, (row, col) in enumerate(((row1, col1), (row2, col2))):
        bytes_of(row.at[pl.ds(0, 15)], r_send.at[phase])
        bytes_of(col.at[pl.ds(0, 15)], c_send.at[phase])
    bytes_of(norms.at[pl.ds(0, N - 1)], n_send)
    bytes_of(gj.at[pl.ds(0, quarter)], g_send)
    bytes_of(gi.at[pl.ds(0, 22 * PIECE - 8 * PIECE)], g_send)
    bytes_of(gj.at[pl.ds(0, 8 * PIECE)], g_send)

    @pl.when(swapped)
    def _():
        bytes_of(g_own, g_send)

    @pl.when(i != tj)
    def _():
        bytes_of(g_own, g_send)

    @pl.when(swapped)
    def _():
        r_swap.wait_send()
        r_swap.wait_recv()
        r_out[...] = r_far[...]


def store(s_ref, r_ref, s_hbm, r_hbm, sems):
    copies = [
        pltpu.make_async_copy(s_ref, s_hbm, sems.at[0]),
        pltpu.make_async_copy(r_ref, r_hbm, sems.at[1]),
    ]
    for copy in copies:
        copy.start()
    for copy in copies:
        copy.wait()


def local(gradient, stat_old):
    dma = pltpu.SemaphoreType.DMA
    n_col, n_row = len(COL_KEYS), len(ROW_KEYS)
    block = jax.ShapeDtypeStruct((B, B), jnp.float32)
    tile = pltpu.VMEM((B, B), jnp.float32)
    panel = pltpu.VMEM((N, B, B), jnp.float32)
    pieces = pltpu.VMEM((N * PIECE, B), jnp.float32)
    made = pl.pallas_call(
        kernel,
        out_shape=(block, block),
        in_specs=[pl.BlockSpec(memory_space=pltpu.HBM)] * 2,
        out_specs=[pl.BlockSpec(memory_space=pltpu.VMEM)] * 2,
        scratch_shapes=[
            pltpu.VMEM((PIECE, B), jnp.float32), tile, tile, tile, tile, tile,
            pieces, pieces, panel, panel, panel, panel, pltpu.VMEM((N, 1, B), jnp.float32),
            dma((3,)), dma(()), dma(()), dma(()), dma(()),
            dma((2,)), dma((2,)), dma((n_col,)), dma((n_row,)), dma((n_col,)), dma((n_row,)),
            dma(()), dma(()), dma((3,)), dma((3,)),
        ],
        compiler_params=pltpu.CompilerParams(
            collective_id=0, has_side_effects=True, vmem_limit_bytes=16 * 1024 * 1024
        ),
        name="shampoo",
    )(
        pltpu.with_memory_space_constraint(gradient.T, pltpu.HBM),
        pltpu.with_memory_space_constraint(stat_old, pltpu.HBM),
    )
    return pl.pallas_call(
        store,
        out_shape=(block, block),
        in_specs=[pl.BlockSpec(memory_space=pltpu.VMEM)] * 2,
        out_specs=[pl.BlockSpec(memory_space=pltpu.HBM)] * 2,
        scratch_shapes=[dma((2,))],
        compiler_params=pltpu.CompilerParams(vmem_limit_bytes=1024 * 1024),
        name="store",
    )(*made)


def solution(mesh):
    placed = (P("gx", "gy"), P("gx", "gy"))
    return jax.shard_map(local, mesh=mesh, in_specs=placed, out_specs=placed, check_vma=False)
```
